8 devices in a mesh: col: 4 (over z, y, x), row: 2 (over core).
Axes of the slice: x: 2, y: 2, z: 1, core: 2. Of those that a mesh axis runs over, the one named last changes fastest.
Arguments:
- vel_u: float32 [30, 128, 2048], P(None, 'row', 'col')
- vel_v: float32 [30, 128, 2048], P(None, 'row', 'col')
- temperature: float32 [30, 128, 2048], P(None, 'row', 'col')
- salinity: float32 [30, 128, 2048], P(None, 'row', 'col')
- surf_eta: float32 [128, 2048], P('row', 'col')
- trans_u: float32 [128, 2048], P('row', 'col')
- trans_v: float32 [128, 2048], P('row', 'col')
- bottom_depth: float32 [128, 2048], P('row', 'col')
- level_count: int32 [128, 2048], P('row', 'col')
- avg_weights: float32 [30], replicated
Outputs:
- output 1: float32 [128, 2048], P('row', 'col')
- output 2: float32 [128, 2048], P('row', 'col')
- output 3: float32 [128, 2048], P('row', 'col')
- output 4: float32 [30, 128, 2048], P(None, 'row', 'col')
- output 5: float32 [30, 128, 2048], P(None, 'row', 'col')
- output 6: float32 [30, 128, 2048], P(None, 'row', 'col')
- output 7: float32 [30, 128, 2048], P(None, 'row', 'col')
All inputs are finite; a program needn't handle non-finite values.
Results may differ from the reference program's by a relative error of at most 0.001.
Values sent between devices are 32-bit elements.
A program may use at most 1 GiB of HBM per device.

```python
import jax
import jax.numpy as jnp
from jax import lax

LEVELS = 30
SUBCYCLES = 30
GRID_Y = 128
GRID_X = 2048

TIME_STEP = 1.0
GRAVITY = 16.0
BC_GRAVITY = 4.0
EXPAND_T = 0.2
CONTRACT_S = 0.6
CORIO_F0 = 0.4
CORIO_BETA = 0.4
VISC_R = 2.0
DIFF_R = 0.5


def setup_inputs(seed: int = 0) -> dict:
    keys = jax.random.split(jax.random.key(seed), 10)
    shape3 = (LEVELS, GRID_Y, GRID_X)
    shape2 = (GRID_Y, GRID_X)
    north_open = (jnp.arange(GRID_Y) < GRID_Y - 1).astype(jnp.float32)[:, None]
    vel_u = 0.3 * jax.random.normal(keys[0], shape3, jnp.float32)
    vel_v = 0.3 * jax.random.normal(keys[1], shape3, jnp.float32) * north_open
    temperature = jax.random.normal(keys[2], shape3, jnp.float32)
    salinity = 0.5 * jax.random.normal(keys[3], shape3, jnp.float32)
    surf_eta = 0.1 * jax.random.normal(keys[4], shape2, jnp.float32)
    trans_u = 0.3 * jax.random.normal(keys[5], shape2, jnp.float32)
    trans_v = 0.3 * jax.random.normal(keys[6], shape2, jnp.float32) * north_open
    bottom_depth = jax.random.uniform(keys[7], shape2, jnp.float32, 0.5, 1.5)
    level_count = jax.random.randint(keys[8], shape2, 1, LEVELS + 1, dtype=jnp.int32)
    level_count = level_count.at[0, 0].set(1).at[0, 1].set(LEVELS)
    ramp = (jnp.arange(SUBCYCLES) + 1.0) / SUBCYCLES
    raw_weights = ramp * jax.random.uniform(keys[9], (SUBCYCLES,), jnp.float32, 0.5, 1.5)
    avg_weights = raw_weights / jnp.sum(raw_weights)
    return {'vel_u': vel_u, 'vel_v': vel_v, 'temperature': temperature, 'salinity': salinity, 'surf_eta': surf_eta, 'trans_u': trans_u, 'trans_v': trans_v, 'bottom_depth': bottom_depth, 'level_count': level_count, 'avg_weights': avg_weights}


def pad_halo(field):
    wrapped = jnp.concatenate([field[..., -1:], field, field[..., :1]], axis=-1)
    ghost = jnp.zeros_like(wrapped[..., :1, :])
    return jnp.concatenate([ghost, wrapped, ghost], axis=-2)


def shifted(padded, step_y, step_x):
    n_rows = padded.shape[-2] - 2
    n_cols = padded.shape[-1] - 2
    return padded[..., 1 + step_y:1 + step_y + n_rows, 1 + step_x:1 + step_x + n_cols]


def tri_solve(right_side, active, strength):
    link = strength * active[1:]
    zero_row = jnp.zeros_like(right_side[:1])
    low_links = jnp.concatenate([zero_row, link], axis=0)
    up_links = jnp.concatenate([link, zero_row], axis=0)

    def down(carry, level):
        ratio_prev, value_prev = carry
        low_link, up_link, target = level
        denominator = 1.0 + low_link + up_link + low_link * ratio_prev
        ratio = -up_link / denominator
        value = (target + low_link * value_prev) / denominator
        return (ratio, value), (ratio, value)

    start = (jnp.zeros_like(right_side[0]), jnp.zeros_like(right_side[0]))
    _, (ratios, values) = lax.scan(down, start, (low_links, up_links, right_side))

    def back(below, level):
        ratio, value = level
        solved = value - ratio * below
        return solved, solved

    _, solved_all = lax.scan(back, jnp.zeros_like(right_side[0]), (ratios, values), reverse=True)
    return solved_all


def ocean_columns(u_pad, v_pad, temperature_pad, salinity_pad, count_pad, depth_pad, coriolis_u, coriolis_v):
    n_levels = u_pad.shape[0]
    count_mid = shifted(count_pad, 0, 0)
    levels_u = jnp.minimum(count_mid, shifted(count_pad, 0, 1))
    levels_uw = jnp.minimum(shifted(count_pad, 0, -1), count_mid)
    levels_v = jnp.minimum(count_mid, shifted(count_pad, 1, 0))
    levels_vs = jnp.minimum(shifted(count_pad, -1, 0), count_mid)
    level_index = jnp.arange(n_levels)[:, None, None]
    mask_mid = (level_index < count_mid).astype(jnp.float32)
    mask_u = (level_index < levels_u).astype(jnp.float32)
    mask_uw = (level_index < levels_uw).astype(jnp.float32)
    mask_v = (level_index < levels_v).astype(jnp.float32)
    mask_vs = (level_index < levels_vs).astype(jnp.float32)
    u_mid = shifted(u_pad, 0, 0)
    v_mid = shifted(v_pad, 0, 0)
    u_west = shifted(u_pad, 0, -1)
    v_south = shifted(v_pad, -1, 0)
    v_at_u = 0.25 * (v_mid + shifted(v_pad, 0, 1) + v_south + shifted(v_pad, -1, 1))
    u_at_v = 0.25 * (u_mid + u_west + shifted(u_pad, 1, 0) + shifted(u_pad, 1, -1))
    inertia_u = 0.5 * (u_mid * (shifted(u_pad, 0, 1) - u_west) + v_at_u * (shifted(u_pad, 1, 0) - shifted(u_pad, -1, 0)))
    inertia_v = 0.5 * (u_at_v * (shifted(v_pad, 0, 1) - shifted(v_pad, 0, -1)) + v_mid * (shifted(v_pad, 1, 0) - v_south))
    density = CONTRACT_S * salinity_pad - EXPAND_T * temperature_pad
    pressure = (BC_GRAVITY / n_levels) * (jnp.cumsum(density, axis=0) - 0.5 * density)
    pressure_mid = shifted(pressure, 0, 0)
    u_star = u_mid + TIME_STEP * (coriolis_u * v_at_u - inertia_u - shifted(pressure, 0, 1) + pressure_mid)
    v_star = v_mid + TIME_STEP * (-coriolis_v * u_at_v - inertia_v - shifted(pressure, 1, 0) + pressure_mid)
    u_visc = tri_solve(u_star, mask_u, VISC_R)
    v_visc = tri_solve(v_star, mask_v, VISC_R)
    count_u = jnp.maximum(jnp.sum(mask_u, axis=0), 1.0)
    count_v = jnp.maximum(jnp.sum(mask_v, axis=0), 1.0)
    depth_mid = shifted(depth_pad, 0, 0)
    depth_u = 0.5 * (depth_mid + shifted(depth_pad, 0, 1))
    depth_v = 0.5 * (depth_mid + shifted(depth_pad, 1, 0))
    force_u = depth_u * jnp.sum(mask_u * (u_visc - u_mid), axis=0) / count_u / TIME_STEP
    force_v = depth_v * jnp.sum(mask_v * (v_visc - v_mid), axis=0) / count_v / TIME_STEP
    shear_u = u_visc - jnp.sum(mask_u * u_visc, axis=0) / count_u
    shear_v = v_visc - jnp.sum(mask_v * v_visc, axis=0) / count_v
    wet_u = (levels_u > 0).astype(jnp.float32)
    wet_v = (levels_v > 0).astype(jnp.float32)

    def advect(tracer_pad):
        tracer_mid = shifted(tracer_pad, 0, 0)
        flux_east = mask_u * u_mid * (tracer_mid + shifted(tracer_pad, 0, 1))
        flux_west = mask_uw * u_west * (shifted(tracer_pad, 0, -1) + tracer_mid)
        flux_north = mask_v * v_mid * (tracer_mid + shifted(tracer_pad, 1, 0))
        flux_south = mask_vs * v_south * (shifted(tracer_pad, -1, 0) + tracer_mid)
        return tracer_mid - 0.5 * TIME_STEP * (flux_east - flux_west + flux_north - flux_south)

    temperature_new = tri_solve(advect(temperature_pad), mask_mid, DIFF_R)
    salinity_new = tri_solve(advect(salinity_pad), mask_mid, DIFF_R)
    return (shear_u, shear_v, mask_u, mask_v, depth_u, depth_v, wet_u, wet_v, force_u, force_v, temperature_new, salinity_new)


def fast_update(stack_pad, force_u, force_v, depth_u, depth_v, wet_u, wet_v, coriolis_u, coriolis_v, dt_fast):
    eta_pad = stack_pad[0]
    trans_u_pad = stack_pad[1]
    trans_v_pad = stack_pad[2]
    eta_ext = eta_pad[1:, 1:] - dt_fast * (trans_u_pad[1:, 1:] - trans_u_pad[1:, :-1] + trans_v_pad[1:, 1:] - trans_v_pad[:-1, 1:])
    eta_new = eta_ext[:-1, :-1]
    trans_u_old = shifted(trans_u_pad, 0, 0)
    trans_v_old = shifted(trans_v_pad, 0, 0)
    v_at_u = 0.25 * (trans_v_old + shifted(trans_v_pad, 0, 1) + shifted(trans_v_pad, -1, 0) + shifted(trans_v_pad, -1, 1))
    u_at_v = 0.25 * (trans_u_old + shifted(trans_u_pad, 0, -1) + shifted(trans_u_pad, 1, 0) + shifted(trans_u_pad, 1, -1))
    trans_u_new = wet_u * (trans_u_old + dt_fast * (coriolis_u * v_at_u + force_u - GRAVITY * depth_u * (eta_ext[:-1, 1:] - eta_new)))
    trans_v_new = wet_v * (trans_v_old + dt_fast * (force_v - coriolis_v * u_at_v - GRAVITY * depth_v * (eta_ext[1:, :-1] - eta_new)))
    return eta_new, trans_u_new, trans_v_new


def reference(vel_u, vel_v, temperature, salinity, surf_eta, trans_u, trans_v, bottom_depth, level_count, avg_weights):
    n_rows = surf_eta.shape[0]
    dt_fast = TIME_STEP / avg_weights.shape[0]
    row_pos = jnp.arange(n_rows).astype(jnp.float32)[:, None]
    coriolis_u = CORIO_F0 + CORIO_BETA * ((row_pos + 0.5) / n_rows - 0.5)
    coriolis_v = CORIO_F0 + CORIO_BETA * ((row_pos + 1.0) / n_rows - 0.5)
    columns = ocean_columns(pad_halo(vel_u), pad_halo(vel_v), pad_halo(temperature), pad_halo(salinity), pad_halo(level_count), pad_halo(bottom_depth), coriolis_u, coriolis_v)
    shear_u, shear_v, mask_u, mask_v, depth_u, depth_v, wet_u, wet_v, force_u, force_v, temperature_new, salinity_new = columns

    def subcycle(carry, weight):
        eta_old, trans_u_old, trans_v_old, acc_u, acc_v = carry
        stack_pad = pad_halo(jnp.stack([eta_old, trans_u_old, trans_v_old]))
        eta_new, trans_u_new, trans_v_new = fast_update(stack_pad, force_u, force_v, depth_u, depth_v, wet_u, wet_v, coriolis_u, coriolis_v, dt_fast)
        return (eta_new, trans_u_new, trans_v_new, acc_u + weight * trans_u_new, acc_v + weight * trans_v_new), None

    zero_field = jnp.zeros_like(surf_eta)
    final, _ = lax.scan(subcycle, (surf_eta, trans_u, trans_v, zero_field, zero_field), avg_weights)
    eta_fin, trans_u_fin, trans_v_fin, bar_u, bar_v = final
    vel_u_new = mask_u * (shear_u + bar_u / depth_u)
    vel_v_new = mask_v * (shear_v + bar_v / depth_v)
    return (eta_fin, trans_u_fin, trans_v_fin, vel_u_new, vel_v_new, temperature_new, salinity_new)
```

```python
import functools

import jax
import jax.numpy as jnp
from jax import lax
from jax.experimental import pallas as pl
from jax.experimental.pallas import tpu as pltpu
from jax.sharding import PartitionSpec as P

TIME_STEP = 1.0
GRAVITY = 16.0
BC_GRAVITY = 4.0
EXPAND_T = 0.2
CONTRACT_S = 0.6
CORIO_F0 = 0.4
CORIO_BETA = 0.4
VISC_R = 2.0
DIFF_R = 0.5

MESH = pl.DeviceIdType.MESH
SL = 8
LN = 128
LEVELS = 30
NR = 64
NC = 4
HY = 32
HX = 32
EXT = NR + HY
PAD = SL
EROWS = EXT + 2 * PAD
STRIPS = EXT // SL
LANE_COUNT = 4 * LEVELS
LANE_DEPTH = LANE_COUNT + 1


def elimination(strength):
    pivots, ends = [], []
    for level in range(LEVELS):
        below = strength * strength / pivots[-1] if level else strength
        pivots.append(1.0 + 2.0 * strength - below)
        ends.append(1.0 + strength - below)
    inverse = [1.0 / pivot for pivot in pivots]
    carry = [strength / pivot for pivot in pivots]
    ending = [pivot / end for pivot, end in zip(pivots, ends)]
    return inverse, carry, ending


INV_V, CARRY_V, END_V = elimination(VISC_R)
INV_D, CARRY_D, END_D = elimination(DIFF_R)


def roll_e(x):
    return pltpu.roll(x, 127, x.ndim - 1)


def roll_w(x):
    return pltpu.roll(x, 1, x.ndim - 1)


def turn(x, amount):
    amount = amount % LN
    return pltpu.roll(x, amount, x.ndim - 1) if amount else x


def following(x):
    return jnp.concatenate([x[1:], x[:1]], axis=0)


def preceding(x):
    return jnp.concatenate([x[-1:], x[:-1]], axis=0)


def step_kernel(n_col, wts, u_h, v_h, t_h, s_h, eta_h, tu_h, tv_h, dep_h, cnt_h,
                vu, vv, vt, vs, aux,
                ub, vb, tb, sb, eta, ua, ubt, va, vbt, dep, cnt, cnt_i, fx, fy,
                au, av, bu, bv, cu, cv, mu, mv, accu, accv, meanu, meanv,
                pk, pkl, rx, rxl,
                sem_in, sem_2d, sem_rs, sem_rr, sem_fs, sem_fr, sem_xs, sem_xr, sem_ls, sem_lr, sem_gs, sem_gr):
    col = lax.axis_index('col')
    row = lax.axis_index('row')
    east = lax.rem(col + 1, n_col)
    west = lax.rem(col + n_col - 1, n_col)
    other = 1 - row
    own = pl.multiple_of(PAD + HY * row, SL)
    near = pl.multiple_of(HY * other, SL)
    far = pl.multiple_of(PAD + NR * row, SL)
    mid = PAD + HY
    lane = lax.broadcasted_iota(jnp.int32, (SL, LN), 1)
    sub = lax.broadcasted_iota(jnp.int32, (SL, LN), 0)
    cubes = ((u_h, ub), (v_h, vb), (t_h, tb), (s_h, sb))
    flats = ((eta_h, eta), (tu_h, ua), (tv_h, va), (dep_h, dep), (cnt_h, cnt_i))

    loads = {}
    for c in (0, 3, 1, 2):
        for f, (src, dst) in enumerate(cubes):
            loads[f, c] = pltpu.make_async_copy(
                src.at[:, :, pl.ds(c * LN, LN)], dst.at[:, c, pl.ds(SL, NR), :], sem_in.at[f, c])
    flat_loads = []
    for f, (src, dst) in enumerate(flats):
        for c in range(NC):
            flat_loads.append(pltpu.make_async_copy(
                src.at[:, pl.ds(c * LN, LN)], dst.at[c, pl.ds(own, NR), :], sem_2d.at[f, c]))
    for c in (0, 3):
        for f in range(4):
            loads[f, c].start()
    for copy in flat_loads:
        copy.start()
    for c in (1, 2):
        for f in range(4):
            loads[f, c].start()

    barrier = pltpu.get_barrier_semaphore()
    for peer in ({'col': east, 'row': row}, {'col': west, 'row': row}, {'col': col, 'row': other},
                 {'col': east, 'row': other}, {'col': west, 'row': other}):
        pl.semaphore_signal(barrier, inc=1, device_id=peer, device_id_type=MESH)

    wall = pl.multiple_of((NR + SL) * row, SL)
    zero4 = jnp.zeros((NC, SL, LN), jnp.float32)

    @pl.loop(0, LEVELS)
    def _(k):
        for _, dst in cubes:
            dst[k, 0:NC, pl.ds(wall, SL), :] = zero4

    zero5 = jnp.zeros((NC + 1, SL, LN), jnp.float32)
    for start in (0, PAD + EXT):
        for ref in (eta, ua, ubt, va, vbt, dep, cnt, fx, fy):
            ref[:, pl.ds(start, SL), :] = zero5
        cnt_i[:, pl.ds(start, SL), :] = jnp.zeros((NC, SL, LN), jnp.int32)
        for d in range(2):
            for p in range(2):
                rx[d, p, pl.ds(start, SL), :] = jnp.zeros((SL, LN), jnp.float32)

    pl.semaphore_wait(barrier, 5)

    row_copies = []
    edge_src = pl.multiple_of((NR - SL) * other, SL)
    for f, (src, dst) in enumerate(cubes):
        for c in range(NC):
            row_copies.append(pltpu.make_async_remote_copy(
                src_ref=src.at[:, pl.ds(edge_src, SL), pl.ds(c * LN, LN)],
                dst_ref=dst.at[:, c, pl.ds(wall, SL), :],
                send_sem=sem_rs.at[f, c], recv_sem=sem_rr.at[f, c],
                device_id={'col': col, 'row': other}, device_id_type=MESH))
    flat_copies = []
    for f, (src, dst) in enumerate(flats):
        for c in range(NC):
            flat_copies.append(pltpu.make_async_remote_copy(
                src_ref=src.at[pl.ds(near, HY), pl.ds(c * LN, LN)],
                dst_ref=dst.at[c, pl.ds(far, HY), :],
                send_sem=sem_fs.at[f, c], recv_sem=sem_fr.at[f, c],
                device_id={'col': col, 'row': other}, device_id_type=MESH))
    for copy in row_copies + flat_copies:
        copy.start()

    zero1 = jnp.zeros((SL, LN), jnp.float32)
    for f, (_, buf) in enumerate(cubes):
        loads[f, 0].wait()
        loads[f, 3].wait()

        @pl.loop(0, NR // 16)
        def _(q):
            for half_q in range(2):
                r = 2 * q + half_q
                rows = pl.ds(pl.multiple_of(SL + SL * r, SL), SL)
                rows_o = pl.ds(pl.multiple_of(SL * r, SL), SL)
                acc_e = zero1 if f == 0 else pk[0, 0, rows_o, :]
                acc_w = zero1 if f == 0 else pk[1, 0, rows_o, :]
                for k in range(LEVELS):
                    m = f * LEVELS + k
                    acc_e = jnp.where(lane == (m - 1) % LN, turn(buf[k, NC - 1, rows, :], m), acc_e)
                    acc_w = jnp.where(lane == m, turn(buf[k, 0, rows, :], m), acc_w)
                pk[0, 0, rows_o, :] = acc_e
                pk[1, 0, rows_o, :] = acc_w

    for copy in flat_loads:
        copy.wait()

    @pl.loop(0, NR // SL)
    def _(r):
        rows_e = pl.ds(pl.multiple_of(own + SL * r, SL), SL)
        rows_o = pl.ds(pl.multiple_of(SL * r, SL), SL)
        acc_e = pk[0, 0, rows_o, :]
        acc_w = pk[1, 0, rows_o, :]
        for m, ref in ((LANE_COUNT, cnt_i), (LANE_DEPTH, dep)):
            acc_e = jnp.where(lane == m - 1, turn(ref[NC - 1, rows_e, :].astype(jnp.float32), m), acc_e)
            acc_w = jnp.where(lane == m, turn(ref[0, rows_e, :].astype(jnp.float32), m), acc_w)
        pk[0, 0, rows_o, :] = acc_e
        pk[1, 0, rows_o, :] = acc_w
        acc_e = turn(eta[NC - 1, rows_e, :], HX)
        acc_w = eta[0, rows_e, :]
        for p, ref in ((1, ua), (2, va), (3, dep)):
            here = lane >= p * HX
            acc_e = jnp.where(here, turn(ref[NC - 1, rows_e, :], HX * (p + 1)), acc_e)
            acc_w = jnp.where(here, turn(ref[0, rows_e, :], HX * p), acc_w)
        pk[0, 1, rows_o, :] = acc_e
        pk[1, 1, rows_o, :] = acc_w

    for copy in flat_copies:
        copy.wait_recv()
    for r in range(STRIPS):
        cnt[0:NC, pl.ds(PAD + SL * r, SL), :] = cnt_i[:, pl.ds(PAD + SL * r, SL), :].astype(jnp.float32)

    x_copies = []
    for d, side in ((0, east), (1, west)):
        x_copies.append(pltpu.make_async_remote_copy(
            src_ref=pk.at[d], dst_ref=rx.at[d, :, pl.ds(own, NR), :],
            send_sem=sem_xs.at[d, 0], recv_sem=sem_xr.at[d, 0],
            device_id={'col': side, 'row': row}, device_id_type=MESH))
        x_copies.append(pltpu.make_async_remote_copy(
            src_ref=pk.at[d, :, pl.ds(near, HY), :], dst_ref=rx.at[d, :, pl.ds(far, HY), :],
            send_sem=sem_xs.at[d, 1], recv_sem=sem_xr.at[d, 1],
            device_id={'col': side, 'row': other}, device_id_type=MESH))
    for copy in x_copies:
        copy.start()

    for c in (1, 2):
        for f in range(4):
            loads[f, c].wait()
    for copy in row_copies:
        copy.wait_recv()

    half = 0.5 * BC_GRAVITY / LEVELS
    first0 = lax.broadcasted_iota(jnp.int32, (1, SL, LN), 2) == 0
    last127 = lax.broadcasted_iota(jnp.int32, (1, SL, LN), 2) == 127

    def shift_e(mine, following_tile):
        return roll_e(jnp.where(first0, following_tile, mine))

    def shift_w(mine, preceding_tile):
        return roll_w(jnp.where(last127, preceding_tile, mine))

    def ring_e(x):
        return shift_e(x, following(x))

    def ring_w(x):
        return shift_w(x, preceding(x))

    def inner(x):
        return x[1:3], x[2:4], x[0:2]

    def outer(x):
        return (jnp.concatenate([x[0:1], x[3:4]], axis=0), jnp.concatenate([x[1:2], x[4:5]], axis=0),
                jnp.concatenate([x[4:5], x[2:3]], axis=0))

    def every(x):
        return x[0:4], x[1:5], jnp.concatenate([x[4:5], x[0:3]], axis=0)

    def momentum(r, tiles, places):
        rb = pl.multiple_of(SL + SL * r, SL)
        eb = pl.multiple_of(own + SL * r, SL)
        out = pl.ds(pl.multiple_of(SL * r, SL), SL)
        y = (NR * row + SL * r + sub).astype(jnp.float32)
        fu4 = 0.25 * (CORIO_F0 + CORIO_BETA * ((y + 0.5) / (2 * NR) - 0.5))
        fv4 = 0.25 * (CORIO_F0 + CORIO_BETA * ((y + 1.0) / (2 * NR) - 0.5))

        def load(ref, k, dr=0):
            return ref[k, :, pl.ds(rb + dr, SL), :]

        def put(ref, rows, value):
            for i, c in enumerate(places):
                ref[c, rows, :] = value[i]

        count, count_e, _ = tiles(cnt[:, pl.ds(eb, SL), :])
        lu = jnp.minimum(count, shift_e(count, count_e))
        lv = jnp.minimum(count, tiles(cnt[:, pl.ds(eb + 1, SL), :])[0])
        qx = qy = su = sv = sdu = sdv = jnp.zeros((len(places), SL, LN), jnp.float32)
        wu = wv = None
        for k in range(LEVELS):
            u, ue, uw = tiles(load(ub, k))
            un, _, unw = tiles(load(ub, k, 1))
            us = tiles(load(ub, k, -1))[0]
            v, ve, vw = tiles(load(vb, k))
            vn = tiles(load(vb, k, 1))[0]
            vso, vse, _ = tiles(load(vb, k, -1))
            s0, s_e, _ = tiles(load(sb, k))
            t0, t_e, _ = tiles(load(tb, k))
            rho = (CONTRACT_S * half) * s0 - (EXPAND_T * half) * t0
            rho_e = (CONTRACT_S * half) * s_e - (EXPAND_T * half) * t_e
            rho_n = (CONTRACT_S * half) * tiles(load(sb, k, 1))[0] - (EXPAND_T * half) * tiles(load(tb, k, 1))[0]
            w2 = v + vso
            w4 = w2 + shift_e(w2, ve + vse)
            y2 = u + un
            y4 = y2 + shift_w(y2, uw + unw)
            dx = shift_e(rho, rho_e) - rho
            dy = rho_n - rho
            px = qx + dx
            qx = px + dx
            py = qy + dy
            qy = py + dy
            du = w4 * (fu4 - 0.125 * (un - us)) - (0.5 * u) * (shift_e(u, ue) - shift_w(u, uw)) - px
            dv = -(y4 * (fv4 + 0.125 * (shift_e(v, ve) - shift_w(v, vw))) + (0.5 * v) * (vn - vso) + py)
            on_u = lu > float(k)
            on_v = lv > float(k)
            su = su + jnp.where(on_u, u, 0.0)
            sv = sv + jnp.where(on_v, v, 0.0)
            sdu = sdu + jnp.where(on_u, du, 0.0)
            sdv = sdv + jnp.where(on_v, dv, 0.0)
            tu, tv = u + du, v + dv
            wu = INV_V[k] * (tu if k == 0 else tu + VISC_R * wu)
            wv = INV_V[k] * (tv if k == 0 else tv + VISC_R * wv)
            put(vu.at[k], out, wu)
            put(vv.at[k], out, wv)
        inv_u = 1.0 / jnp.maximum(lu, 1.0)
        inv_v = 1.0 / jnp.maximum(lv, 1.0)
        depth, depth_e, _ = tiles(dep[:, pl.ds(eb, SL), :])
        hu = 0.5 * (depth + shift_e(depth, depth_e))
        hv = 0.5 * (depth + tiles(dep[:, pl.ds(eb + 1, SL), :])[0])
        put(fx, pl.ds(eb, SL), hu * (sdu * inv_u) / TIME_STEP)
        put(fy, pl.ds(eb, SL), hv * (sdv * inv_v) / TIME_STEP)
        put(meanu, out, (su + sdu) * inv_u)
        put(meanv, out, (sv + sdv) * inv_v)
        put(aux.at[0], out, count)
        put(aux.at[1], out, lu)
        put(aux.at[2], out, lv)

    def tracers(r):
        rb = pl.multiple_of(SL + SL * r, SL)
        eb = pl.multiple_of(own + SL * r, SL)
        out = pl.ds(pl.multiple_of(SL * r, SL), SL)

        def load(ref, k, dr=0):
            return ref[k, :, pl.ds(rb + dr, SL), :]

        count, count_e, count_w = every(cnt[:, pl.ds(eb, SL), :])
        lu = jnp.minimum(count, shift_e(count, count_e))
        luw = jnp.minimum(count, shift_w(count, count_w))
        lv = jnp.minimum(count, cnt[0:NC, pl.ds(eb + 1, SL), :])
        lvs = jnp.minimum(count, cnt[0:NC, pl.ds(eb - 1, SL), :])
        half_dt = 0.5 * TIME_STEP
        carried = [None, None]
        for k in range(LEVELS):
            level = float(k)
            u, _, uw = every(load(ub, k))
            ge = jnp.where(lu > level, half_dt * u, 0.0)
            gw = jnp.where(luw > level, half_dt * shift_w(u, uw), 0.0)
            gn = jnp.where(lv > level, half_dt * load(vb, k)[:NC], 0.0)
            gs = jnp.where(lvs > level, half_dt * load(vb, k, -1)[:NC], 0.0)
            keep = 1.0 - (ge - gw + gn - gs)
            inside = count > level
            for i, (buf, dst) in enumerate(((tb, vt), (sb, vs))):
                q, qe, qw = every(load(buf, k))
                new = keep * q - (ge * shift_e(q, qe) - gw * shift_w(q, qw)
                                  + gn * load(buf, k, 1)[:NC] - gs * load(buf, k, -1)[:NC])
                w = INV_D[k] * (new if k == 0 else new + DIFF_R * carried[i])
                carried[i] = w
                dst[k, :, out, :] = jnp.where(inside, w, new)

    @pl.loop(0, NR // SL)
    def _(r):
        momentum(r, inner, (1, 2))

    for copy in x_copies:
        copy.wait_recv()

    even = lax.rem(lane, 2) == 0

    def unpack(r):
        eb = pl.multiple_of(own + SL * r, SL)
        from_west, from_east = rx[0, 0, pl.ds(eb, SL), :], rx[1, 0, pl.ds(eb, SL), :]
        return jnp.where(even, from_east, from_west), jnp.where(even, from_west, from_east)

    @pl.loop(0, NR // SL + 2)
    def _(q):
        r = q - 1
        merged = unpack(r)
        rows = pl.ds(pl.multiple_of(SL * q, SL), SL)
        for f, (_, buf) in enumerate(cubes):
            for k in range(LEVELS):
                m = f * LEVELS + k
                buf[k, NC, rows, :] = turn(merged[m % 2], -m)
        rows = pl.ds(pl.multiple_of(own + SL * r, SL), SL)
        cnt[NC, rows, :] = turn(merged[LANE_COUNT % 2], -LANE_COUNT)
        dep[NC, rows, :] = turn(merged[LANE_DEPTH % 2], -LANE_DEPTH)

    @pl.loop(0, NR // SL)
    def _(r):
        momentum(r, outer, (0, 3))

    for r in range(NR // SL):
        rows_e = pl.ds(pl.multiple_of(own + SL * r, SL), SL)
        acc_e = turn(fx[NC - 1, rows_e, :], HX)
        acc_w = fx[0, rows_e, :]
        for p, ref in ((1, fy), (2, cnt)):
            here = lane >= p * HX
            acc_e = jnp.where(here, turn(ref[NC - 1, rows_e, :], HX * (p + 1)), acc_e)
            acc_w = jnp.where(here, turn(ref[0, rows_e, :], HX * p), acc_w)
        pkl[0, pl.ds(SL * r, SL), :] = acc_e
        pkl[1, pl.ds(SL * r, SL), :] = acc_w

    late = []
    for f, ref in enumerate((fx, fy)):
        late.append(pltpu.make_async_remote_copy(
            src_ref=ref.at[pl.ds(0, NC), pl.ds(mid, HY), :], dst_ref=ref.at[pl.ds(0, NC), pl.ds(far, HY), :],
            send_sem=sem_gs.at[f], recv_sem=sem_gr.at[f],
            device_id={'col': col, 'row': other}, device_id_type=MESH))
    for d, side in ((0, east), (1, west)):
        late.append(pltpu.make_async_remote_copy(
            src_ref=pkl.at[d], dst_ref=rxl.at[d, pl.ds(own, NR), :],
            send_sem=sem_ls.at[d, 0], recv_sem=sem_lr.at[d, 0],
            device_id={'col': side, 'row': row}, device_id_type=MESH))
        late.append(pltpu.make_async_remote_copy(
            src_ref=pkl.at[d, pl.ds(near, HY), :], dst_ref=rxl.at[d, pl.ds(far, HY), :],
            send_sem=sem_ls.at[d, 1], recv_sem=sem_lr.at[d, 1],
            device_id={'col': side, 'row': other}, device_id_type=MESH))
    for copy in late:
        copy.start()

    @pl.loop(0, NR // SL)
    def _(r):
        tracers(r)

    for copy in late:
        copy.wait_recv()

    def strip(r, dr=0):
        return pl.ds(PAD + SL * r + dr, SL)

    for r in range(STRIPS):
        for p, ref, src in ((0, eta, 1), (1, ua, 1), (2, va, 1), (3, dep, 1), (0, fx, 2), (1, fy, 2), (2, cnt, 2)):
            from_east = rx[1, 1, strip(r), :] if src == 1 else rxl[1, strip(r), :]
            from_west = rx[0, 1, strip(r), :] if src == 1 else rxl[0, strip(r), :]
            ref[NC, strip(r), :] = jnp.where(
                lane < HX, turn(from_east, -HX * p),
                jnp.where(lane >= LN - HX, turn(from_west, LN - HX - HX * p), 0.0))

    dt_fast = TIME_STEP / LEVELS
    for r in range(STRIPS):
        y = (HY * row + SL * r + sub).astype(jnp.float32)
        f_u = CORIO_F0 + CORIO_BETA * ((y + 0.5) / (2 * NR) - 0.5)
        f_v = CORIO_F0 + CORIO_BETA * ((y + 1.0) / (2 * NR) - 0.5)
        rows = strip(r)
        count, depth = cnt[:, rows, :], dep[:, rows, :]
        wet_u = (jnp.minimum(count, ring_e(count)) > 0.0).astype(jnp.float32)
        wet_v = (jnp.minimum(count, cnt[:, strip(r, 1), :]) > 0.0).astype(jnp.float32)
        mu[:, rows, :] = wet_u
        mv[:, rows, :] = wet_v
        au[:, rows, :] = wet_u * (0.25 * dt_fast * f_u)
        av[:, rows, :] = wet_v * (0.25 * dt_fast * f_v)
        bu[:, rows, :] = wet_u * (dt_fast * dt_fast) * fx[:, rows, :]
        bv[:, rows, :] = wet_v * (dt_fast * dt_fast) * fy[:, rows, :]
        scale = 0.5 * GRAVITY * dt_fast * dt_fast
        cu[:, rows, :] = wet_u * (scale * (depth + ring_e(depth)))
        cv[:, rows, :] = wet_v * (scale * (depth + dep[:, strip(r, 1), :]))
        ua[:, rows, :] = dt_fast * ua[:, rows, :]
        va[:, rows, :] = dt_fast * va[:, rows, :]
        accu[:, pl.ds(SL * r, SL), :] = jnp.zeros((NC, SL, LN), jnp.float32)
        accv[:, pl.ds(SL * r, SL), :] = jnp.zeros((NC, SL, LN), jnp.float32)

    def subcycle(n, u_old, v_old, u_new, v_new, first):
        weight = wts[n]
        for r in range(STRIPS):
            rows = strip(r)
            u = u_old[:, rows, :]
            eta[:, rows, :] = eta[:, rows, :] - (u - ring_w(u) + v_old[:, rows, :] - v_old[:, strip(r, -1), :])
        for r in range(STRIPS):
            rows = strip(r)
            u, v, e = u_old[:, rows, :], v_old[:, rows, :], eta[:, rows, :]
            w2 = v + v_old[:, strip(r, -1), :]
            y2 = u + u_old[:, strip(r, 1), :]
            if first:
                u, v = mu[:, rows, :] * u, mv[:, rows, :] * v
            u = u + (au[:, rows, :] * (w2 + ring_e(w2)) + bu[:, rows, :] - cu[:, rows, :] * (ring_e(e) - e))
            v = v + (bv[:, rows, :] - av[:, rows, :] * (y2 + ring_w(y2)) - cv[:, rows, :] * (eta[:, strip(r, 1), :] - e))
            u_new[:, rows, :] = u
            v_new[:, rows, :] = v
            rows_a = pl.ds(SL * r, SL)
            accu[:, rows_a, :] = accu[:, rows_a, :] + weight * u[:NC]
            accv[:, rows_a, :] = accv[:, rows_a, :] + weight * v[:NC]

    subcycle(0, ua, va, ubt, vbt, True)
    subcycle(1, ubt, vbt, ua, va, False)

    @pl.loop(1, LEVELS // 2)
    def _(pair):
        subcycle(2 * pair, ua, va, ubt, vbt, False)
        subcycle(2 * pair + 1, ubt, vbt, ua, va, False)

    @pl.loop(0, NR // SL)
    def _(r):
        eb = pl.multiple_of(own + SL * r, SL)
        rows = pl.ds(eb, SL)
        rows_a = pl.ds(pl.multiple_of(eb - PAD, SL), SL)
        out = pl.ds(pl.multiple_of(SL * r, SL), SL)
        depth = dep[:, rows, :]
        hu = 0.5 * (depth + ring_e(depth))[:NC]
        hv = 0.5 * (depth + dep[:, pl.ds(eb + 1, SL), :])[:NC]
        aux[3, :, out, :] = LEVELS / TIME_STEP * accu[:, rows_a, :] / hu - meanu[:, out, :]
        aux[4, :, out, :] = LEVELS / TIME_STEP * accv[:, rows_a, :] / hv - meanv[:, out, :]
        aux[5, :, out, :] = eta[0:NC, rows, :]
        aux[6, :, out, :] = (LEVELS / TIME_STEP) * ua[0:NC, rows, :]
        aux[7, :, out, :] = (LEVELS / TIME_STEP) * va[0:NC, rows, :]

    for copy in row_copies + flat_copies + x_copies + late:
        copy.wait_send()


def finish_kernel(vu, vv, vt, vs, aux, o_eta, o_tu, o_tv, o_u, o_v, o_t, o_s):
    for c in range(NC):
        cols = pl.ds(c * LN, LN)
        o_eta[:, cols] = aux[5, c]
        o_tu[:, cols] = aux[6, c]
        o_tv[:, cols] = aux[7, c]
        count, lu, lv = aux[0, c], aux[1, c], aux[2, c]
        gu, gv = aux[3, c], aux[4, c]
        xu = xv = xt = xs = jnp.zeros((SL, LN), jnp.float32)
        for k in reversed(range(LEVELS)):
            level = float(k)
            last = count == level + 1.0
            inside = count > level
            wu, wv, wt, ws = vu[k, c], vv[k, c], vt[k, c], vs[k, c]
            xu = jnp.where(lu == level + 1.0, END_V[k] * wu, wu + CARRY_V[k] * xu)
            xv = jnp.where(lv == level + 1.0, END_V[k] * wv, wv + CARRY_V[k] * xv)
            xt = jnp.where(last, END_D[k] * wt, wt + CARRY_D[k] * xt)
            xs = jnp.where(last, END_D[k] * ws, ws + CARRY_D[k] * xs)
            o_u[k, :, cols] = jnp.where(lu > level, xu + gu, 0.0)
            o_v[k, :, cols] = jnp.where(lv > level, xv + gv, 0.0)
            o_t[k, :, cols] = jnp.where(inside, xt, wt)
            o_s[k, :, cols] = jnp.where(inside, xs, ws)


def solution(mesh):
    n_col = mesh.shape['col']

    def step(vel_u, vel_v, temperature, salinity, surf_eta, trans_u, trans_v, bottom_depth, level_count, avg_weights):
        f32 = jnp.float32
        swept = jax.ShapeDtypeStruct((LEVELS, NC, NR, LN), f32)
        vmem = pl.BlockSpec(memory_space=pltpu.VMEM)
        anywhere = pl.BlockSpec(memory_space=pl.ANY)
        wide = pltpu.VMEM((NC + 1, EROWS, LN), f32)
        cube = pltpu.VMEM((LEVELS, NC + 1, NR + 16, LN), f32)
        acc = pltpu.VMEM((NC, EXT, LN), f32)
        mean = pltpu.VMEM((NC, NR, LN), f32)
        dma = pltpu.SemaphoreType.DMA
        swept_all = pl.pallas_call(
            functools.partial(step_kernel, n_col),
            out_shape=(swept,) * 4 + (jax.ShapeDtypeStruct((SL, NC, NR, LN), f32),),
            in_specs=[pl.BlockSpec(memory_space=pltpu.SMEM)] + [anywhere] * 9,
            out_specs=(vmem,) * 5,
            scratch_shapes=[cube] * 4 + [wide] * 7 + [pltpu.VMEM((NC, EROWS, LN), jnp.int32)] + [wide] * 10
            + [acc, acc, mean, mean,
               pltpu.VMEM((2, 2, NR, LN), f32), pltpu.VMEM((2, NR, LN), f32),
               pltpu.VMEM((2, 2, EROWS, LN), f32), pltpu.VMEM((2, EROWS, LN), f32)]
            + [dma((4, NC)), dma((5, NC)), dma((4, NC)), dma((4, NC)), dma((5, NC)), dma((5, NC)),
               dma((2, 2)), dma((2, 2)), dma((2, 2)), dma((2, 2)), dma((2,)), dma((2,))],
            compiler_params=pltpu.CompilerParams(
                collective_id=0, has_side_effects=True, vmem_limit_bytes=33 * 1024 * 1024),
            name='step_kernel',
        )(avg_weights, *[pltpu.with_memory_space_constraint(x, pltpu.HBM) for x in (vel_u, vel_v, temperature, salinity, surf_eta, trans_u, trans_v, bottom_depth, level_count)])
        flat_out = jax.ShapeDtypeStruct(surf_eta.shape, f32)
        cube_out = jax.ShapeDtypeStruct(vel_u.shape, f32)
        flat_spec = pl.BlockSpec((SL, NC * LN), lambda r: (r, 0))
        cube_spec = pl.BlockSpec((LEVELS, SL, NC * LN), lambda r: (0, r, 0))
        in_spec = pl.BlockSpec((LEVELS, NC, SL, LN), lambda r: (0, 0, r, 0))
        return pl.pallas_call(
            finish_kernel,
            grid=(NR // SL,),
            out_shape=(flat_out,) * 3 + (cube_out,) * 4,
            in_specs=[in_spec] * 4 + [pl.BlockSpec((SL, NC, SL, LN), lambda r: (0, 0, r, 0))],
            out_specs=(flat_spec,) * 3 + (cube_spec,) * 4,
            compiler_params=pltpu.CompilerParams(vmem_limit_bytes=16 * 1024 * 1024),
            name='finish_kernel',
        )(*swept_all)

    cube = P(None, 'row', 'col')
    flat = P('row', 'col')
    return jax.shard_map(step, mesh=mesh, in_specs=(cube, cube, cube, cube, flat, flat, flat, flat, flat, P()), out_specs=(flat, flat, flat, cube, cube, cube, cube), check_vma=False)
```

```python
import functools

import jax
import jax.numpy as jnp
from jax import lax
from jax.experimental import pallas as pl
from jax.experimental.pallas import tpu as pltpu
from jax.sharding import PartitionSpec as P

TIME_STEP = 1.0
GRAVITY = 16.0
BC_GRAVITY = 4.0
EXPAND_T = 0.2
CONTRACT_S = 0.6
CORIO_F0 = 0.4
CORIO_BETA = 0.4
VISC_R = 2.0
DIFF_R = 0.5

MESH = pl.DeviceIdType.MESH
SL = 8
LN = 128
LEVELS = 30
NR = 64
NC = 4
HY = 32
HX = 32
EXT = NR + HY
PAD = SL
EROWS = EXT + 2 * PAD
STRIPS = EXT // SL
LANE_COUNT = 4 * LEVELS
LANE_DEPTH = LANE_COUNT + 1


def elimination(strength):
    pivots, ends = [], []
    for level in range(LEVELS):
        below = strength * strength / pivots[-1] if level else strength
        pivots.append(1.0 + 2.0 * strength - below)
        ends.append(1.0 + strength - below)
    inverse = [1.0 / pivot for pivot in pivots]
    carry = [strength / pivot for pivot in pivots]
    ending = [pivot / end for pivot, end in zip(pivots, ends)]
    return inverse, carry, ending


INV_V, CARRY_V, END_V = elimination(VISC_R)
INV_D, CARRY_D, END_D = elimination(DIFF_R)


def roll_e(x):
    return pltpu.roll(x, 127, x.ndim - 1)


def roll_w(x):
    return pltpu.roll(x, 1, x.ndim - 1)


def turn(x, amount):
    amount = amount % LN
    return pltpu.roll(x, amount, x.ndim - 1) if amount else x


def following(x):
    return jnp.concatenate([x[1:], x[:1]], axis=0)


def preceding(x):
    return jnp.concatenate([x[-1:], x[:-1]], axis=0)


def step_kernel(n_col, wts_h, u_h, v_h, t_h, s_h, eta_h, tu_h, tv_h, dep_h, cnt_h,
                vu, vv, vt, vs, aux,
                ub, vb, tb, sb, eta, ua, ubt, va, vbt, dep, cnt, cnt_i, fx, fy,
                au, av, bu, bv, cu, cv, mu, mv, accu, accv, meanu, meanv,
                pk, pkl, rx, rxl, pkw, rxw, wts, sem_w, sem_half,
                sem_in, sem_2d, sem_rs, sem_rr, sem_fs, sem_fr, sem_xs, sem_xr, sem_ls, sem_lr, sem_ws, sem_wr, sem_gs, sem_gr):
    col = lax.axis_index('col')
    row = lax.axis_index('row')
    east = lax.rem(col + 1, n_col)
    west = lax.rem(col + n_col - 1, n_col)
    other = 1 - row
    own = pl.multiple_of(PAD + HY * row, SL)
    near = pl.multiple_of(HY * other, SL)
    far = pl.multiple_of(PAD + NR * row, SL)
    mid = PAD + HY
    lane = lax.broadcasted_iota(jnp.int32, (SL, LN), 1)
    sub = lax.broadcasted_iota(jnp.int32, (SL, LN), 0)
    cubes = ((u_h, ub), (v_h, vb), (t_h, tb), (s_h, sb))
    flats = ((eta_h, eta), (tu_h, ua), (tv_h, va), (dep_h, dep), (cnt_h, cnt_i))

    loads = {}
    part = NR // 2
    for c in range(1, NC - 1):
        for f, (src, dst) in enumerate(cubes):
            for h in range(2):
                loads[f, c, h] = pltpu.make_async_copy(
                    src.at[:, pl.ds(part * h, part), pl.ds(c * LN, LN)],
                    dst.at[:, c, pl.ds(SL + part * h, part), :], sem_half.at[f, c - 1, h])
    for c in (0, NC - 1):
        for f, (src, dst) in enumerate(cubes):
            loads[f, c] = pltpu.make_async_copy(
                src.at[:, :, pl.ds(c * LN, LN)], dst.at[:, c, pl.ds(SL, NR), :], sem_in.at[f, c])
    flat_loads = []
    for f, (src, dst) in enumerate(flats):
        for c in range(NC):
            flat_loads.append(pltpu.make_async_copy(
                src.at[:, pl.ds(c * LN, LN)], dst.at[c, pl.ds(own, NR), :], sem_2d.at[f, c]))
    for c in (0, 3):
        for f in range(4):
            loads[f, c].start()
    for copy in flat_loads:
        copy.start()
    weight_load = pltpu.make_async_copy(wts_h, wts, sem_w)
    weight_load.start()

    barrier = pltpu.get_barrier_semaphore()
    for peer in ({'col': east, 'row': row}, {'col': west, 'row': row}, {'col': col, 'row': other},
                 {'col': east, 'row': other}, {'col': west, 'row': other}):
        pl.semaphore_signal(barrier, inc=1, device_id=peer, device_id_type=MESH)

    wall = pl.multiple_of((NR + SL) * row, SL)
    zero4 = jnp.zeros((NC, SL, LN), jnp.float32)

    @pl.loop(0, LEVELS)
    def _(k):
        for _, dst in cubes:
            dst[k, 0:NC, pl.ds(wall, SL), :] = zero4

    zero5 = jnp.zeros((NC + 1, SL, LN), jnp.float32)
    for start in (0, PAD + EXT):
        for ref in (eta, ua, ubt, va, vbt, dep, cnt, fx, fy):
            ref[:, pl.ds(start, SL), :] = zero5
        cnt_i[:, pl.ds(start, SL), :] = jnp.zeros((NC, SL, LN), jnp.int32)
        rx[:, pl.ds(start, SL), :] = jnp.zeros((2, SL, LN), jnp.float32)

    pl.semaphore_wait(barrier, 5)

    row_copies = []
    edge_src = pl.multiple_of((NR - SL) * other, SL)
    for f, (src, dst) in enumerate(cubes):
        for c in range(NC):
            row_copies.append(pltpu.make_async_remote_copy(
                src_ref=src.at[:, pl.ds(edge_src, SL), pl.ds(c * LN, LN)],
                dst_ref=dst.at[:, c, pl.ds(wall, SL), :],
                send_sem=sem_rs.at[f, c], recv_sem=sem_rr.at[f, c],
                device_id={'col': col, 'row': other}, device_id_type=MESH))
    flat_copies = []
    for f, (src, dst) in enumerate(flats):
        for c in range(NC):
            flat_copies.append(pltpu.make_async_remote_copy(
                src_ref=src.at[pl.ds(near, HY), pl.ds(c * LN, LN)],
                dst_ref=dst.at[c, pl.ds(far, HY), :],
                send_sem=sem_fs.at[f, c], recv_sem=sem_fr.at[f, c],
                device_id={'col': col, 'row': other}, device_id_type=MESH))
    for copy in row_copies + flat_copies:
        copy.start()

    groups = (NR // SL, SL, LN)
    lanes = lax.broadcasted_iota(jnp.int32, (1, SL, LN), 2)
    acc_e = acc_w = jnp.zeros(groups, jnp.float32)
    for f, (_, buf) in enumerate(cubes):
        loads[f, 0].wait()
        loads[f, NC - 1].wait()
        for c in range(1, NC - 1):
            loads[f, c, 0].start()
        for k in range(LEVELS):
            m = f * LEVELS + k
            acc_e = jnp.where(lanes == (m - 1) % LN, turn(buf[k, NC - 1, pl.ds(SL, NR), :].reshape(groups), m), acc_e)
            acc_w = jnp.where(lanes == m, turn(buf[k, 0, pl.ds(SL, NR), :].reshape(groups), m), acc_w)
    for f in range(len(cubes)):
        for c in range(1, NC - 1):
            loads[f, c, 1].start()

    for copy in flat_loads:
        copy.wait()
    for m, ref in ((LANE_COUNT, cnt_i), (LANE_DEPTH, dep)):
        last = ref[NC - 1, pl.ds(own, NR), :].astype(jnp.float32).reshape(groups)
        first = ref[0, pl.ds(own, NR), :].astype(jnp.float32).reshape(groups)
        acc_e = jnp.where(lanes == m - 1, turn(last, m), acc_e)
        acc_w = jnp.where(lanes == m, turn(first, m), acc_w)
    pk[0] = acc_e.reshape(NR, LN)
    pk[1] = acc_w.reshape(NR, LN)

    def side_by_side(dst, refs):
        for r in range(NR // SL):
            rows_e = pl.ds(pl.multiple_of(own + SL * r, SL), SL)
            acc_e = turn(refs[0][NC - 1, rows_e, :], HX)
            acc_w = refs[0][0, rows_e, :]
            for p, ref in enumerate(refs[1:], 1):
                here = lane >= p * HX
                acc_e = jnp.where(here, turn(ref[NC - 1, rows_e, :], HX * (p + 1)), acc_e)
                acc_w = jnp.where(here, turn(ref[0, rows_e, :], HX * p), acc_w)
            dst[0, pl.ds(SL * r, SL), :] = acc_e
            dst[1, pl.ds(SL * r, SL), :] = acc_w

    def sideways(src, dst, sends, recvs, from_row, to_row, rows):
        copies = []
        for d, side in enumerate((east, west)):
            copies.append(pltpu.make_async_remote_copy(
                src_ref=src.at[d], dst_ref=dst.at[d, pl.ds(own, NR), :],
                send_sem=sends.at[d, 0], recv_sem=recvs.at[d, 0],
                device_id={'col': side, 'row': row}, device_id_type=MESH))
            copies.append(pltpu.make_async_remote_copy(
                src_ref=src.at[d, pl.ds(from_row, rows), :], dst_ref=dst.at[d, pl.ds(to_row, rows), :],
                send_sem=sends.at[d, 1], recv_sem=recvs.at[d, 1],
                device_id={'col': side, 'row': other}, device_id_type=MESH))
        return copies

    corner = pl.multiple_of(PAD + HY - SL + (NR - HY + SL) * row, SL)
    x_copies = sideways(pk, rx, sem_xs, sem_xr, edge_src, corner, SL)
    for copy in x_copies:
        copy.start()
    side_by_side(pkw, (eta, ua, va, dep))

    for copy in flat_copies:
        copy.wait_recv()
    for r in range(STRIPS):
        cnt[0:NC, pl.ds(PAD + SL * r, SL), :] = cnt_i[:, pl.ds(PAD + SL * r, SL), :].astype(jnp.float32)


    def inner_half(h):
        for c in range(1, NC - 1):
            for f in range(len(cubes)):
                loads[f, c, h].wait()

    inner_half(0)
    w_copies = sideways(pkw, rxw, sem_ws, sem_wr, near, far, HY)
    for copy in w_copies:
        copy.start()
    for copy in row_copies:
        copy.wait_recv()

    half = 0.5 * BC_GRAVITY / LEVELS
    first0 = lax.broadcasted_iota(jnp.int32, (1, SL, LN), 2) == 0
    last127 = lax.broadcasted_iota(jnp.int32, (1, SL, LN), 2) == 127

    def shift_e(mine, following_tile):
        return roll_e(jnp.where(first0, following_tile, mine))

    def shift_w(mine, preceding_tile):
        return roll_w(jnp.where(last127, preceding_tile, mine))

    def ring_e(x):
        return shift_e(x, following(x))

    def ring_w(x):
        return shift_w(x, preceding(x))

    def inner(x):
        return x[1:3], x[2:4], x[0:2]

    def outer(x):
        return (jnp.concatenate([x[0:1], x[3:4]], axis=0), jnp.concatenate([x[1:2], x[4:5]], axis=0),
                jnp.concatenate([x[4:5], x[2:3]], axis=0))

    def every(x):
        return x[0:4], x[1:5], jnp.concatenate([x[4:5], x[0:3]], axis=0)

    def momentum(r, tiles, places):
        rb = pl.multiple_of(SL + SL * r, SL)
        eb = pl.multiple_of(own + SL * r, SL)
        out = pl.ds(pl.multiple_of(SL * r, SL), SL)
        y = (NR * row + SL * r + sub).astype(jnp.float32)
        fu4 = 0.25 * (CORIO_F0 + CORIO_BETA * ((y + 0.5) / (2 * NR) - 0.5))
        fv4 = 0.25 * (CORIO_F0 + CORIO_BETA * ((y + 1.0) / (2 * NR) - 0.5))

        def load(ref, k, dr=0):
            return ref[k, :, pl.ds(rb + dr, SL), :]

        def put(ref, rows, value):
            for i, c in enumerate(places):
                ref[c, rows, :] = value[i]

        count, count_e, _ = tiles(cnt[:, pl.ds(eb, SL), :])
        lu = jnp.minimum(count, shift_e(count, count_e))
        lv = jnp.minimum(count, tiles(cnt[:, pl.ds(eb + 1, SL), :])[0])
        qx = qy = su = sv = sdu = sdv = jnp.zeros((len(places), SL, LN), jnp.float32)
        wu = wv = None
        for k in range(LEVELS):
            u, ue, uw = tiles(load(ub, k))
            un, _, unw = tiles(load(ub, k, 1))
            us = tiles(load(ub, k, -1))[0]
            v, ve, vw = tiles(load(vb, k))
            vn = tiles(load(vb, k, 1))[0]
            vso, vse, _ = tiles(load(vb, k, -1))
            s0, s_e, _ = tiles(load(sb, k))
            t0, t_e, _ = tiles(load(tb, k))
            rho = (CONTRACT_S * half) * s0 - (EXPAND_T * half) * t0
            rho_e = (CONTRACT_S * half) * s_e - (EXPAND_T * half) * t_e
            rho_n = (CONTRACT_S * half) * tiles(load(sb, k, 1))[0] - (EXPAND_T * half) * tiles(load(tb, k, 1))[0]
            w2 = v + vso
            w4 = w2 + shift_e(w2, ve + vse)
            y2 = u + un
            y4 = y2 + shift_w(y2, uw + unw)
            dx = shift_e(rho, rho_e) - rho
            dy = rho_n - rho
            px = qx + dx
            qx = px + dx
            py = qy + dy
            qy = py + dy
            du = w4 * (fu4 - 0.125 * (un - us)) - (0.5 * u) * (shift_e(u, ue) - shift_w(u, uw)) - px
            dv = -(y4 * (fv4 + 0.125 * (shift_e(v, ve) - shift_w(v, vw))) + (0.5 * v) * (vn - vso) + py)
            on_u = lu > float(k)
            on_v = lv > float(k)
            su = su + jnp.where(on_u, u, 0.0)
            sv = sv + jnp.where(on_v, v, 0.0)
            sdu = sdu + jnp.where(on_u, du, 0.0)
            sdv = sdv + jnp.where(on_v, dv, 0.0)
            tu, tv = u + du, v + dv
            wu = INV_V[k] * (tu if k == 0 else tu + VISC_R * wu)
            wv = INV_V[k] * (tv if k == 0 else tv + VISC_R * wv)
            put(vu.at[k], out, wu)
            put(vv.at[k], out, wv)
        inv_u = 1.0 / jnp.maximum(lu, 1.0)
        inv_v = 1.0 / jnp.maximum(lv, 1.0)
        depth, depth_e, _ = tiles(dep[:, pl.ds(eb, SL), :])
        hu = 0.5 * (depth + shift_e(depth, depth_e))
        hv = 0.5 * (depth + tiles(dep[:, pl.ds(eb + 1, SL), :])[0])
        put(fx, pl.ds(eb, SL), hu * (sdu * inv_u) / TIME_STEP)
        put(fy, pl.ds(eb, SL), hv * (sdv * inv_v) / TIME_STEP)
        put(meanu, out, (su + sdu) * inv_u)
        put(meanv, out, (sv + sdv) * inv_v)
        put(aux.at[0], out, count)
        put(aux.at[1], out, lu)
        put(aux.at[2], out, lv)

    def tracers(r):
        rb = pl.multiple_of(SL + SL * r, SL)
        eb = pl.multiple_of(own + SL * r, SL)
        out = pl.ds(pl.multiple_of(SL * r, SL), SL)

        def load(ref, k, dr=0):
            return ref[k, :, pl.ds(rb + dr, SL), :]

        count = cnt[:, pl.ds(eb, SL), :]
        lu = jnp.minimum(count, ring_e(count))
        count = count[:NC]
        lv = jnp.minimum(count, cnt[0:NC, pl.ds(eb + 1, SL), :])
        lvs = jnp.minimum(count, cnt[0:NC, pl.ds(eb - 1, SL), :])
        carried = [None, None]
        inside = count > 0.0
        for k in range(LEVELS):
            level = float(k)
            ge = TIME_STEP * jnp.where(lu > level, load(ub, k), 0.0)
            ge, _, gw = every(ge)
            gw = shift_w(ge, gw)
            gn = TIME_STEP * jnp.where(lv > level, load(vb, k)[:NC], 0.0)
            gs = TIME_STEP * jnp.where(lvs > level, load(vb, k, -1)[:NC], 0.0)
            keep = 2.0 - (ge - gw + gn - gs)
            inside_next = count > level + 1.0
            ending = 0.5 * INV_D[k] * END_D[k]
            pivot = ending if k == LEVELS - 1 else jnp.where(inside_next, 0.5 * INV_D[k], ending)
            for i, (buf, dst) in enumerate(((tb, vt), (sb, vs))):
                q, qe, qw = every(load(buf, k))
                twice = keep * q - (ge * shift_e(q, qe) - gw * shift_w(q, qw)
                                    + gn * load(buf, k, 1)[:NC] - gs * load(buf, k, -1)[:NC])
                w = pivot * (twice if k == 0 else twice + 2.0 * DIFF_R * carried[i])
                carried[i] = w
                dst[k, :, out, :] = jnp.where(inside, w, q)
            inside = inside_next

    @pl.loop(0, NR // SL)
    def _(r):
        @pl.when(r == part // SL - 1)
        def _():
            inner_half(1)

        momentum(r, inner, (1, 2))

    for copy in x_copies:
        copy.wait_recv()

    def unpack(rows, shape):
        even = lax.rem(lanes if len(shape) == 3 else lane, 2) == 0
        from_west, from_east = rx[0, rows, :].reshape(shape), rx[1, rows, :].reshape(shape)
        return jnp.where(even, from_east, from_west), jnp.where(even, from_west, from_east)

    def unpack_cube(f, rows, merged):
        for k in range(LEVELS):
            m = f * LEVELS + k
            cubes[f][1][k, NC, rows, :] = turn(merged[m % 2], -m).reshape(rows.size, LN)

    merged = unpack(pl.ds(own, NR), groups)
    for f in range(len(cubes)):
        unpack_cube(f, pl.ds(SL, NR), merged)
    cnt[NC, pl.ds(own, NR), :] = turn(merged[LANE_COUNT % 2], -LANE_COUNT).reshape(NR, LN)
    dep[NC, pl.ds(own, NR), :] = turn(merged[LANE_DEPTH % 2], -LANE_DEPTH).reshape(NR, LN)
    unpack_cube(1, pl.ds(0, SL), unpack(pl.ds(pl.multiple_of(own - SL, SL), SL), (SL, LN)))
    unpack_cube(0, pl.ds(SL + NR, SL), unpack(pl.ds(pl.multiple_of(own + NR, SL), SL), (SL, LN)))

    @pl.loop(0, NR // SL)
    def _(r):
        momentum(r, outer, (0, 3))

    side_by_side(pkl, (fx, fy, cnt))

    late = []
    for f, ref in enumerate((fx, fy)):
        late.append(pltpu.make_async_remote_copy(
            src_ref=ref.at[pl.ds(0, NC), pl.ds(mid, HY), :], dst_ref=ref.at[pl.ds(0, NC), pl.ds(far, HY), :],
            send_sem=sem_gs.at[f], recv_sem=sem_gr.at[f],
            device_id={'col': col, 'row': other}, device_id_type=MESH))
    late += sideways(pkl, rxl, sem_ls, sem_lr, near, far, HY)
    for copy in late:
        copy.start()

    @pl.loop(0, NR // SL)
    def _(r):
        tracers(r)

    for copy in w_copies + late:
        copy.wait_recv()
    weight_load.wait()

    def strip(r, dr=0):
        return pl.ds(PAD + SL * r + dr, SL)

    for r in range(STRIPS):
        for p, ref, src in ((0, eta, 1), (1, ua, 1), (2, va, 1), (3, dep, 1), (0, fx, 2), (1, fy, 2), (2, cnt, 2)):
            from_east = rxw[1, strip(r), :] if src == 1 else rxl[1, strip(r), :]
            from_west = rxw[0, strip(r), :] if src == 1 else rxl[0, strip(r), :]
            ref[NC, strip(r), :] = jnp.where(
                lane < HX, turn(from_east, -HX * p),
                jnp.where(lane >= LN - HX, turn(from_west, LN - HX - HX * p), 0.0))

    dt_fast = TIME_STEP / LEVELS
    for r in range(STRIPS):
        y = (HY * row + SL * r + sub).astype(jnp.float32)
        f_u = CORIO_F0 + CORIO_BETA * ((y + 0.5) / (2 * NR) - 0.5)
        f_v = CORIO_F0 + CORIO_BETA * ((y + 1.0) / (2 * NR) - 0.5)
        rows = strip(r)
        count, depth = cnt[:, rows, :], dep[:, rows, :]
        wet_u = (jnp.minimum(count, ring_e(count)) > 0.0).astype(jnp.float32)
        wet_v = (jnp.minimum(count, cnt[:, strip(r, 1), :]) > 0.0).astype(jnp.float32)
        mu[:, rows, :] = wet_u
        mv[:, rows, :] = wet_v
        au[:, rows, :] = wet_u * (0.25 * dt_fast * f_u)
        av[:, rows, :] = wet_v * (0.25 * dt_fast * f_v)
        bu[:, rows, :] = wet_u * (dt_fast * dt_fast) * fx[:, rows, :]
        bv[:, rows, :] = wet_v * (dt_fast * dt_fast) * fy[:, rows, :]
        scale = 0.5 * GRAVITY * dt_fast * dt_fast
        cu[:, rows, :] = wet_u * (scale * (depth + ring_e(depth)))
        cv[:, rows, :] = wet_v * (scale * (depth + dep[:, strip(r, 1), :]))
        ua[:, rows, :] = dt_fast * ua[:, rows, :]
        va[:, rows, :] = dt_fast * va[:, rows, :]
        accu[:, pl.ds(SL * r, SL), :] = jnp.zeros((NC, SL, LN), jnp.float32)
        accv[:, pl.ds(SL * r, SL), :] = jnp.zeros((NC, SL, LN), jnp.float32)

    def subcycle(n, u_old, v_old, u_new, v_new, span, first):
        weight = wts[n]
        weight_old = wts[jnp.maximum(n - 1, 0)]
        for r in span:
            rows = strip(r)
            u = u_old[:, rows, :]
            eta[:, rows, :] = eta[:, rows, :] - (u - ring_w(u) + v_old[:, rows, :] - v_old[:, strip(r, -1), :])
        for r in span:
            rows, rows_a = strip(r), pl.ds(SL * r, SL)
            u, v, e = u_old[:, rows, :], v_old[:, rows, :], eta[:, rows, :]
            w2 = v + v_old[:, strip(r, -1), :]
            y2 = u + u_old[:, strip(r, 1), :]
            ug, vg = (mu[:, rows, :] * u, mv[:, rows, :] * v) if first else (u, v)
            un = ug + (au[:, rows, :] * (w2 + ring_e(w2)) + bu[:, rows, :] - cu[:, rows, :] * (ring_e(e) - e))
            vn = vg + (bv[:, rows, :] - av[:, rows, :] * (y2 + ring_w(y2))
                       - cv[:, rows, :] * (eta[:, strip(r, 1), :] - e))
            u_new[:, rows, :] = un
            v_new[:, rows, :] = vn
            if u_new is ua:
                accu[:, rows_a, :] = accu[:, rows_a, :] + (weight_old * u[:NC] + weight * un[:NC])
                accv[:, rows_a, :] = accv[:, rows_a, :] + (weight_old * v[:NC] + weight * vn[:NC])

    def pair_of(pair, span, first):
        subcycle(2 * pair, ua, va, ubt, vbt, span, first)
        subcycle(2 * pair + 1, ubt, vbt, ua, va, span, False)

    pair_of(0, range(STRIPS), True)

    narrow = STRIPS - 2
    turning = (SL * (STRIPS - narrow) - 2) // 2

    @pl.loop(1, turning)
    def _(pair):
        pair_of(pair, range(STRIPS), False)

    @pl.when(row == 0)
    def _():
        @pl.loop(turning, LEVELS // 2)
        def _(pair):
            pair_of(pair, range(narrow), False)

    @pl.when(row == 1)
    def _():
        @pl.loop(turning, LEVELS // 2)
        def _(pair):
            pair_of(pair, range(STRIPS - narrow, STRIPS), False)

    @pl.loop(0, NR // SL)
    def _(r):
        eb = pl.multiple_of(own + SL * r, SL)
        rows = pl.ds(eb, SL)
        rows_a = pl.ds(pl.multiple_of(eb - PAD, SL), SL)
        out = pl.ds(pl.multiple_of(SL * r, SL), SL)
        depth = dep[:, rows, :]
        hu = 0.5 * (depth + ring_e(depth))[:NC]
        hv = 0.5 * (depth + dep[:, pl.ds(eb + 1, SL), :])[:NC]
        aux[3, :, out, :] = LEVELS / TIME_STEP * accu[:, rows_a, :] / hu - meanu[:, out, :]
        aux[4, :, out, :] = LEVELS / TIME_STEP * accv[:, rows_a, :] / hv - meanv[:, out, :]
        aux[5, :, out, :] = eta[0:NC, rows, :]
        aux[6, :, out, :] = (LEVELS / TIME_STEP) * ua[0:NC, rows, :]
        aux[7, :, out, :] = (LEVELS / TIME_STEP) * va[0:NC, rows, :]

    for copy in row_copies + flat_copies + x_copies + w_copies + late:
        copy.wait_send()


def finish_kernel(vu, vv, vt, vs, aux, o_eta, o_tu, o_tv, o_u, o_v, o_t, o_s, *scratch):
    flat_bufs, cube_bufs, sem_f, sem_c = scratch[:3], scratch[3:7], scratch[7], scratch[8]
    flat_copies = []
    for i, (buf, ref) in enumerate(zip(flat_bufs, (o_eta, o_tu, o_tv))):
        for c in range(NC):
            buf[:, pl.ds(c * LN, LN)] = aux[5 + i, c]
        flat_copies.append(pltpu.make_async_copy(buf, ref, sem_f.at[i]))

    def copies(r):
        rows = pl.ds(SL * r if isinstance(r, int) else pl.multiple_of(SL * r, SL), SL)
        return [pltpu.make_async_copy(buf.at[:, rows, :], ref.at[:, rows, :], sem_c.at[i, r])
                for i, (buf, ref) in enumerate(zip(cube_bufs, (o_u, o_v, o_t, o_s)))]

    @pl.loop(0, NR // SL)
    def _(r):
        finish_rows(pl.ds(pl.multiple_of(SL * r, SL), SL), vu, vv, vt, vs, aux, *cube_bufs)
        for copy in copies(r):
            copy.start()

    for copy in flat_copies:
        copy.start()
    for r in range(NR // SL):
        for copy in copies(r):
            copy.wait()
    for copy in flat_copies:
        copy.wait()


def finish_rows(rows, vu, vv, vt, vs, aux, o_u, o_v, o_t, o_s):
    def put(ref, value):
        for c in range(NC):
            ref[rows, pl.ds(c * LN, LN)] = value[c]

    count, lu, lv, gu, gv = (aux[i, :, rows, :] for i in range(5))
    xu = xv = xt = xs = on_u = on_v = inside = None
    for k in reversed(range(LEVELS)):
        level = float(k)
        wu, wv, xt_new, xs_new = (ref[k, :, rows, :] for ref in (vu, vv, vt, vs))
        if k == LEVELS - 1:
            xu, xv = END_V[k] * wu, END_V[k] * wv
        else:
            xu = jnp.where(on_u, wu + CARRY_V[k] * xu, END_V[k] * wu)
            xv = jnp.where(on_v, wv + CARRY_V[k] * xv, END_V[k] * wv)
            xt_new = xt_new + CARRY_D[k] * jnp.where(inside, xt, 0.0)
            xs_new = xs_new + CARRY_D[k] * jnp.where(inside, xs, 0.0)
        xt, xs = xt_new, xs_new
        on_u, on_v, inside = lu > level, lv > level, count > level
        put(o_u.at[k], jnp.where(on_u, xu + gu, 0.0))
        put(o_v.at[k], jnp.where(on_v, xv + gv, 0.0))
        put(o_t.at[k], xt)
        put(o_s.at[k], xs)


def solution(mesh):
    n_col = mesh.shape['col']

    def step(vel_u, vel_v, temperature, salinity, surf_eta, trans_u, trans_v, bottom_depth, level_count, avg_weights):
        f32 = jnp.float32
        swept = jax.ShapeDtypeStruct((LEVELS, NC, NR, LN), f32)
        vmem = pl.BlockSpec(memory_space=pltpu.VMEM)
        anywhere = pl.BlockSpec(memory_space=pl.ANY)
        wide = pltpu.VMEM((NC + 1, EROWS, LN), f32)
        cube = pltpu.VMEM((LEVELS, NC + 1, NR + 16, LN), f32)
        acc = pltpu.VMEM((NC, EXT, LN), f32)
        mean = pltpu.VMEM((NC, NR, LN), f32)
        dma = pltpu.SemaphoreType.DMA
        swept_all = pl.pallas_call(
            functools.partial(step_kernel, n_col),
            out_shape=(swept,) * 4 + (jax.ShapeDtypeStruct((SL, NC, NR, LN), f32),),
            in_specs=[anywhere] * 10,
            out_specs=(vmem,) * 5,
            scratch_shapes=[cube] * 4 + [wide] * 7 + [pltpu.VMEM((NC, EROWS, LN), jnp.int32)] + [wide] * 10
            + [acc, acc, mean, mean,
               *[pltpu.VMEM((2, rows, LN), f32) for rows in (NR, NR, EROWS, EROWS, NR, EROWS)],
               pltpu.SMEM((LEVELS,), f32), dma(()), dma((4, NC - 2, 2))]
            + [dma((4, NC)), dma((5, NC)), dma((4, NC)), dma((4, NC)), dma((5, NC)), dma((5, NC)),
               *[dma((2, 2))] * 6, dma((2,)), dma((2,))],
            compiler_params=pltpu.CompilerParams(
                collective_id=0, has_side_effects=True, vmem_limit_bytes=33 * 1024 * 1024),
            name='step_kernel',
        )(*[pltpu.with_memory_space_constraint(x, pltpu.HBM) for x in (avg_weights, vel_u, vel_v, temperature, salinity, surf_eta, trans_u, trans_v, bottom_depth, level_count)])
        flat_out = jax.ShapeDtypeStruct(surf_eta.shape, f32)
        cube_out = jax.ShapeDtypeStruct(vel_u.shape, f32)
        return pl.pallas_call(
            finish_kernel,
            out_shape=(flat_out,) * 3 + (cube_out,) * 4,
            in_specs=[vmem] * 5,
            out_specs=(anywhere,) * 7,
            scratch_shapes=[pltpu.VMEM(surf_eta.shape, f32)] * 3 + [pltpu.VMEM(vel_u.shape, f32)] * 4
            + [dma((3,)), dma((4, NR // SL))],
            compiler_params=pltpu.CompilerParams(vmem_limit_bytes=20 * 1024 * 1024),
            name='finish_kernel',
        )(*swept_all)

    cube = P(None, 'row', 'col')
    flat = P('row', 'col')
    return jax.shard_map(step, mesh=mesh, in_specs=(cube, cube, cube, cube, flat, flat, flat, flat, flat, P()), out_specs=(flat, flat, flat, cube, cube, cube, cube), check_vma=False)
```

```python
import functools

import jax
import jax.numpy as jnp
from jax import lax
from jax.experimental import pallas as pl
from jax.experimental.pallas import tpu as pltpu
from jax.sharding import PartitionSpec as P

TIME_STEP = 1.0
GRAVITY = 16.0
BC_GRAVITY = 4.0
EXPAND_T = 0.2
CONTRACT_S = 0.6
CORIO_F0 = 0.4
CORIO_BETA = 0.4
VISC_R = 2.0
DIFF_R = 0.5

MESH = pl.DeviceIdType.MESH
SL = 8
LN = 128
LEVELS = 30
NR = 64
NC = 4
HY = 32
HX = 32
EXT = NR + HY
PAD = SL
EROWS = EXT + 2 * PAD
STRIPS = EXT // SL
LANE_COUNT = 4 * LEVELS
LANE_DEPTH = LANE_COUNT + 1


def elimination(strength):
    pivots, ends = [], []
    for level in range(LEVELS):
        below = strength * strength / pivots[-1] if level else strength
        pivots.append(1.0 + 2.0 * strength - below)
        ends.append(1.0 + strength - below)
    inverse = [1.0 / pivot for pivot in pivots]
    carry = [strength / pivot for pivot in pivots]
    ending = [pivot / end for pivot, end in zip(pivots, ends)]
    return inverse, carry, ending


INV_V, CARRY_V, END_V = elimination(VISC_R)
INV_D, CARRY_D, END_D = elimination(DIFF_R)


def roll_e(x):
    return pltpu.roll(x, 127, x.ndim - 1)


def roll_w(x):
    return pltpu.roll(x, 1, x.ndim - 1)


def turn(x, amount):
    amount = amount % LN
    return pltpu.roll(x, amount, x.ndim - 1) if amount else x


def following(x):
    return jnp.concatenate([x[1:], x[:1]], axis=0)


def preceding(x):
    return jnp.concatenate([x[-1:], x[:-1]], axis=0)


def step_kernel(n_col, wts_h, u_h, v_h, t_h, s_h, eta_h, tu_h, tv_h, dep_h, cnt_h,
                vu, vv, vt, vs, aux,
                ub, vb, tb, sb, eta, ua, ubt, va, vbt, dep, cnt, cnt_i, fx, fy,
                au, av, bu, bv, cu, cv, mu, mv, accu, accv, meanu, meanv,
                pk, pkl, rx, rxl, pkw, rxw, wts, sem_w, sem_half,
                sem_in, sem_2d, sem_rs, sem_rr, sem_fs, sem_fr, sem_xs, sem_xr, sem_ls, sem_lr, sem_ws, sem_wr, sem_gs, sem_gr):
    col = lax.axis_index('col')
    row = lax.axis_index('row')
    east = lax.rem(col + 1, n_col)
    west = lax.rem(col + n_col - 1, n_col)
    other = 1 - row
    own = pl.multiple_of(PAD + HY * row, SL)
    near = pl.multiple_of(HY * other, SL)
    far = pl.multiple_of(PAD + NR * row, SL)
    mid = PAD + HY
    lane = lax.broadcasted_iota(jnp.int32, (SL, LN), 1)
    sub = lax.broadcasted_iota(jnp.int32, (SL, LN), 0)
    cubes = ((u_h, ub), (v_h, vb), (t_h, tb), (s_h, sb))
    flats = ((eta_h, eta), (tu_h, ua), (tv_h, va), (dep_h, dep), (cnt_h, cnt_i))

    loads = {}
    part = NR // 2
    for c in range(1, NC - 1):
        for f, (src, dst) in enumerate(cubes):
            for h in range(2):
                loads[f, c, h] = pltpu.make_async_copy(
                    src.at[:, pl.ds(part * h, part), pl.ds(c * LN, LN)],
                    dst.at[:, c, pl.ds(SL + part * h, part), :], sem_half.at[f, c - 1, h])
    for c in (0, NC - 1):
        for f, (src, dst) in enumerate(cubes):
            loads[f, c] = pltpu.make_async_copy(
                src.at[:, :, pl.ds(c * LN, LN)], dst.at[:, c, pl.ds(SL, NR), :], sem_in.at[f, c])
    flat_loads = []
    for f, (src, dst) in enumerate(flats):
        for c in range(NC):
            flat_loads.append(pltpu.make_async_copy(
                src.at[:, pl.ds(c * LN, LN)], dst.at[c, pl.ds(own, NR), :], sem_2d.at[f, c]))
    for c in (0, 3):
        for f in range(4):
            loads[f, c].start()
    for copy in flat_loads:
        copy.start()
    for h in range(2):
        for f in range(len(cubes)):
            for c in range(1, NC - 1):
                loads[f, c, h].start()
    weight_load = pltpu.make_async_copy(wts_h, wts, sem_w)
    weight_load.start()

    barrier = pltpu.get_barrier_semaphore()
    for peer in ({'col': east, 'row': row}, {'col': west, 'row': row}, {'col': col, 'row': other},
                 {'col': east, 'row': other}, {'col': west, 'row': other}):
        pl.semaphore_signal(barrier, inc=1, device_id=peer, device_id_type=MESH)

    wall = pl.multiple_of((NR + SL) * row, SL)
    zero4 = jnp.zeros((NC, SL, LN), jnp.float32)

    @pl.loop(0, LEVELS)
    def _(k):
        for _, dst in cubes:
            dst[k, 0:NC, pl.ds(wall, SL), :] = zero4

    zero5 = jnp.zeros((NC + 1, SL, LN), jnp.float32)
    for start in (0, PAD + EXT):
        for ref in (eta, ua, ubt, va, vbt, dep, cnt, fx, fy):
            ref[:, pl.ds(start, SL), :] = zero5
        cnt_i[:, pl.ds(start, SL), :] = jnp.zeros((NC, SL, LN), jnp.int32)
        rx[:, pl.ds(start, SL), :] = jnp.zeros((2, SL, LN), jnp.float32)

    pl.semaphore_wait(barrier, 5)

    row_copies = []
    edge_src = pl.multiple_of((NR - SL) * other, SL)
    for f, (src, dst) in enumerate(cubes):
        for c in range(NC):
            row_copies.append(pltpu.make_async_remote_copy(
                src_ref=src.at[:, pl.ds((NR - 1) * other, 1), pl.ds(c * LN, LN)],
                dst_ref=dst.at[:, c, pl.ds((NR + SL) * row + (SL - 1) * other, 1), :],
                send_sem=sem_rs.at[f, c], recv_sem=sem_rr.at[f, c],
                device_id={'col': col, 'row': other}, device_id_type=MESH))
    flat_copies = []
    for f, (src, dst) in enumerate(flats):
        for c in range(NC):
            flat_copies.append(pltpu.make_async_remote_copy(
                src_ref=src.at[pl.ds(near, HY), pl.ds(c * LN, LN)],
                dst_ref=dst.at[c, pl.ds(far, HY), :],
                send_sem=sem_fs.at[f, c], recv_sem=sem_fr.at[f, c],
                device_id={'col': col, 'row': other}, device_id_type=MESH))
    for copy in row_copies + flat_copies:
        copy.start()

    groups = (NR // SL, SL, LN)
    lanes = lax.broadcasted_iota(jnp.int32, (1, SL, LN), 2)
    acc_e = acc_w = jnp.zeros(groups, jnp.float32)
    for f, (_, buf) in enumerate(cubes):
        loads[f, 0].wait()
        loads[f, NC - 1].wait()
        for k in range(LEVELS):
            m = f * LEVELS + k
            acc_e = jnp.where(lanes == (m - 1) % LN, turn(buf[k, NC - 1, pl.ds(SL, NR), :].reshape(groups), m), acc_e)
            acc_w = jnp.where(lanes == m, turn(buf[k, 0, pl.ds(SL, NR), :].reshape(groups), m), acc_w)
    for copy in flat_loads:
        copy.wait()
    for m, ref in ((LANE_COUNT, cnt_i), (LANE_DEPTH, dep)):
        last = ref[NC - 1, pl.ds(own, NR), :].astype(jnp.float32).reshape(groups)
        first = ref[0, pl.ds(own, NR), :].astype(jnp.float32).reshape(groups)
        acc_e = jnp.where(lanes == m - 1, turn(last, m), acc_e)
        acc_w = jnp.where(lanes == m, turn(first, m), acc_w)
    pk[0] = acc_e.reshape(NR, LN)
    pk[1] = acc_w.reshape(NR, LN)

    def side_by_side(dst, refs):
        for r in range(NR // SL):
            rows_e = pl.ds(pl.multiple_of(own + SL * r, SL), SL)
            acc_e = turn(refs[0][NC - 1, rows_e, :], HX)
            acc_w = refs[0][0, rows_e, :]
            for p, ref in enumerate(refs[1:], 1):
                here = lane >= p * HX
                acc_e = jnp.where(here, turn(ref[NC - 1, rows_e, :], HX * (p + 1)), acc_e)
                acc_w = jnp.where(here, turn(ref[0, rows_e, :], HX * p), acc_w)
            dst[0, pl.ds(SL * r, SL), :] = acc_e
            dst[1, pl.ds(SL * r, SL), :] = acc_w

    def sideways(src, dst, sends, recvs, from_row, to_row, rows):
        copies = []
        for d, side in enumerate((east, west)):
            copies.append(pltpu.make_async_remote_copy(
                src_ref=src.at[d], dst_ref=dst.at[d, pl.ds(own, NR), :],
                send_sem=sends.at[d, 0], recv_sem=recvs.at[d, 0],
                device_id={'col': side, 'row': row}, device_id_type=MESH))
            copies.append(pltpu.make_async_remote_copy(
                src_ref=src.at[d, pl.ds(from_row, rows), :], dst_ref=dst.at[d, pl.ds(to_row, rows), :],
                send_sem=sends.at[d, 1], recv_sem=recvs.at[d, 1],
                device_id={'col': side, 'row': other}, device_id_type=MESH))
        return copies

    corner = pl.multiple_of(PAD + HY - SL + (NR - HY + SL) * row, SL)
    x_copies = sideways(pk, rx, sem_xs, sem_xr, edge_src, corner, SL)
    for copy in x_copies:
        copy.start()
    side_by_side(pkw, (eta, ua, va, dep))

    for copy in flat_copies:
        copy.wait_recv()
    for r in range(STRIPS):
        cnt[0:NC, pl.ds(PAD + SL * r, SL), :] = cnt_i[:, pl.ds(PAD + SL * r, SL), :].astype(jnp.float32)


    def inner_half(h):
        for c in range(1, NC - 1):
            for f in range(len(cubes)):
                loads[f, c, h].wait()

    inner_half(0)
    w_copies = sideways(pkw, rxw, sem_ws, sem_wr, near, far, HY)
    for copy in w_copies:
        copy.start()
    for copy in row_copies:
        copy.wait_recv()

    half = 0.5 * BC_GRAVITY / LEVELS
    first0 = lax.broadcasted_iota(jnp.int32, (1, SL, LN), 2) == 0
    last127 = lax.broadcasted_iota(jnp.int32, (1, SL, LN), 2) == 127

    def shift_e(mine, following_tile):
        return roll_e(jnp.where(first0, following_tile, mine))

    def shift_w(mine, preceding_tile):
        return roll_w(jnp.where(last127, preceding_tile, mine))

    def ring_e(x):
        return shift_e(x, following(x))

    def ring_w(x):
        return shift_w(x, preceding(x))

    def inner(x):
        return x[1:3], x[2:4], x[0:2]

    def outer(x):
        return (jnp.concatenate([x[0:1], x[3:4]], axis=0), jnp.concatenate([x[1:2], x[4:5]], axis=0),
                jnp.concatenate([x[4:5], x[2:3]], axis=0))

    def every(x):
        return x[0:4], x[1:5], jnp.concatenate([x[4:5], x[0:3]], axis=0)

    def momentum(r, tiles, places):
        rb = pl.multiple_of(SL + SL * r, SL)
        eb = pl.multiple_of(own + SL * r, SL)
        out = pl.ds(pl.multiple_of(SL * r, SL), SL)
        y = (NR * row + SL * r + sub).astype(jnp.float32)
        fu4 = 0.25 * (CORIO_F0 + CORIO_BETA * ((y + 0.5) / (2 * NR) - 0.5))
        fv4 = 0.25 * (CORIO_F0 + CORIO_BETA * ((y + 1.0) / (2 * NR) - 0.5))

        def load(ref, k, dr=0):
            return ref[k, :, pl.ds(rb + dr, SL), :]

        def put(ref, rows, value):
            for i, c in enumerate(places):
                ref[c, rows, :] = value[i]

        count, count_e, _ = tiles(cnt[:, pl.ds(eb, SL), :])
        lu = jnp.minimum(count, shift_e(count, count_e))
        lv = jnp.minimum(count, tiles(cnt[:, pl.ds(eb + 1, SL), :])[0])
        qx = qy = su = sv = sdu = sdv = jnp.zeros((len(places), SL, LN), jnp.float32)
        wu = wv = None
        for k in range(LEVELS):
            u, ue, uw = tiles(load(ub, k))
            un, _, unw = tiles(load(ub, k, 1))
            us = tiles(load(ub, k, -1))[0]
            v, ve, vw = tiles(load(vb, k))
            vn = tiles(load(vb, k, 1))[0]
            vso, vse, _ = tiles(load(vb, k, -1))
            s0, s_e, _ = tiles(load(sb, k))
            t0, t_e, _ = tiles(load(tb, k))
            rho = (CONTRACT_S * half) * s0 - (EXPAND_T * half) * t0
            rho_e = (CONTRACT_S * half) * s_e - (EXPAND_T * half) * t_e
            rho_n = (CONTRACT_S * half) * tiles(load(sb, k, 1))[0] - (EXPAND_T * half) * tiles(load(tb, k, 1))[0]
            w2 = v + vso
            w4 = w2 + shift_e(w2, ve + vse)
            y2 = u + un
            y4 = y2 + shift_w(y2, uw + unw)
            dx = shift_e(rho, rho_e) - rho
            dy = rho_n - rho
            px = qx + dx
            qx = px + dx
            py = qy + dy
            qy = py + dy
            du = w4 * (fu4 - 0.125 * (un - us)) - (0.5 * u) * (shift_e(u, ue) - shift_w(u, uw)) - px
            dv = -(y4 * (fv4 + 0.125 * (shift_e(v, ve) - shift_w(v, vw))) + (0.5 * v) * (vn - vso) + py)
            on_u = lu > float(k)
            on_v = lv > float(k)
            su = su + jnp.where(on_u, u, 0.0)
            sv = sv + jnp.where(on_v, v, 0.0)
            sdu = sdu + jnp.where(on_u, du, 0.0)
            sdv = sdv + jnp.where(on_v, dv, 0.0)
            tu, tv = u + du, v + dv
            wu = INV_V[k] * (tu if k == 0 else tu + VISC_R * wu)
            wv = INV_V[k] * (tv if k == 0 else tv + VISC_R * wv)
            put(vu.at[k], out, wu)
            put(vv.at[k], out, wv)
        inv_u = 1.0 / jnp.maximum(lu, 1.0)
        inv_v = 1.0 / jnp.maximum(lv, 1.0)
        depth, depth_e, _ = tiles(dep[:, pl.ds(eb, SL), :])
        hu = 0.5 * (depth + shift_e(depth, depth_e))
        hv = 0.5 * (depth + tiles(dep[:, pl.ds(eb + 1, SL), :])[0])
        put(fx, pl.ds(eb, SL), hu * (sdu * inv_u) / TIME_STEP)
        put(fy, pl.ds(eb, SL), hv * (sdv * inv_v) / TIME_STEP)
        put(meanu, out, (su + sdu) * inv_u)
        put(meanv, out, (sv + sdv) * inv_v)
        put(aux.at[0], out, count)
        put(aux.at[1], out, lu)
        put(aux.at[2], out, lv)

    def tracers(r):
        rb = pl.multiple_of(SL + SL * r, SL)
        eb = pl.multiple_of(own + SL * r, SL)
        out = pl.ds(pl.multiple_of(SL * r, SL), SL)

        def load(ref, k, dr=0):
            return ref[k, :, pl.ds(rb + dr, SL), :]

        count = cnt[:, pl.ds(eb, SL), :]
        lu = jnp.minimum(count, ring_e(count))
        count = count[:NC]
        lv = jnp.minimum(count, cnt[0:NC, pl.ds(eb + 1, SL), :])
        lvs = jnp.minimum(count, cnt[0:NC, pl.ds(eb - 1, SL), :])
        carried = [None, None]
        inside = count > 0.0
        for k in range(LEVELS):
            level = float(k)
            ge = TIME_STEP * jnp.where(lu > level, load(ub, k), 0.0)
            ge, _, gw = every(ge)
            gw = shift_w(ge, gw)
            gn = TIME_STEP * jnp.where(lv > level, load(vb, k)[:NC], 0.0)
            gs = TIME_STEP * jnp.where(lvs > level, load(vb, k, -1)[:NC], 0.0)
            keep = 2.0 - (ge - gw + gn - gs)
            inside_next = count > level + 1.0
            ending = 0.5 * INV_D[k] * END_D[k]
            pivot = ending if k == LEVELS - 1 else jnp.where(inside_next, 0.5 * INV_D[k], ending)
            for i, (buf, dst) in enumerate(((tb, vt), (sb, vs))):
                q, qe, qw = every(load(buf, k))
                twice = keep * q - (ge * shift_e(q, qe) - gw * shift_w(q, qw)
                                    + gn * load(buf, k, 1)[:NC] - gs * load(buf, k, -1)[:NC])
                w = pivot * (twice if k == 0 else twice + 2.0 * DIFF_R * carried[i])
                carried[i] = w
                dst[k, :, out, :] = jnp.where(inside, w, q)
            inside = inside_next

    @pl.loop(0, NR // SL)
    def _(r):
        @pl.when(r == part // SL - 1)
        def _():
            inner_half(1)

        momentum(r, inner, (1, 2))

    for copy in x_copies:
        copy.wait_recv()

    def unpack(rows, shape):
        even = lax.rem(lanes if len(shape) == 3 else lane, 2) == 0
        from_west, from_east = rx[0, rows, :].reshape(shape), rx[1, rows, :].reshape(shape)
        return jnp.where(even, from_east, from_west), jnp.where(even, from_west, from_east)

    def unpack_cube(f, rows, merged):
        for k in range(LEVELS):
            m = f * LEVELS + k
            cubes[f][1][k, NC, rows, :] = turn(merged[m % 2], -m).reshape(rows.size, LN)

    merged = unpack(pl.ds(own, NR), groups)
    for f in range(len(cubes)):
        unpack_cube(f, pl.ds(SL, NR), merged)
    cnt[NC, pl.ds(own, NR), :] = turn(merged[LANE_COUNT % 2], -LANE_COUNT).reshape(NR, LN)
    dep[NC, pl.ds(own, NR), :] = turn(merged[LANE_DEPTH % 2], -LANE_DEPTH).reshape(NR, LN)
    unpack_cube(1, pl.ds(0, SL), unpack(pl.ds(pl.multiple_of(own - SL, SL), SL), (SL, LN)))
    unpack_cube(0, pl.ds(SL + NR, SL), unpack(pl.ds(pl.multiple_of(own + NR, SL), SL), (SL, LN)))

    @pl.loop(0, NR // SL)
    def _(r):
        momentum(r, outer, (0, 3))

    side_by_side(pkl, (fx, fy, cnt))

    late = []
    for f, ref in enumerate((fx, fy)):
        late.append(pltpu.make_async_remote_copy(
            src_ref=ref.at[pl.ds(0, NC), pl.ds(mid, HY), :], dst_ref=ref.at[pl.ds(0, NC), pl.ds(far, HY), :],
            send_sem=sem_gs.at[f], recv_sem=sem_gr.at[f],
            device_id={'col': col, 'row': other}, device_id_type=MESH))
    late += sideways(pkl, rxl, sem_ls, sem_lr, near, far, HY)
    for copy in late:
        copy.start()

    @pl.loop(0, NR // SL)
    def _(r):
        tracers(r)

    for copy in w_copies + late:
        copy.wait_recv()
    weight_load.wait()

    def strip(r, dr=0):
        return pl.ds(PAD + SL * r + dr, SL)

    for r in range(STRIPS):
        for p, ref, src in ((0, eta, 1), (1, ua, 1), (2, va, 1), (3, dep, 1), (0, fx, 2), (1, fy, 2), (2, cnt, 2)):
            from_east = rxw[1, strip(r), :] if src == 1 else rxl[1, strip(r), :]
            from_west = rxw[0, strip(r), :] if src == 1 else rxl[0, strip(r), :]
            ref[NC, strip(r), :] = jnp.where(
                lane < HX, turn(from_east, -HX * p),
                jnp.where(lane >= LN - HX, turn(from_west, LN - HX - HX * p), 0.0))

    dt_fast = TIME_STEP / LEVELS
    for r in range(STRIPS):
        y = (HY * row + SL * r + sub).astype(jnp.float32)
        f_u = CORIO_F0 + CORIO_BETA * ((y + 0.5) / (2 * NR) - 0.5)
        f_v = CORIO_F0 + CORIO_BETA * ((y + 1.0) / (2 * NR) - 0.5)
        rows = strip(r)
        count, depth = cnt[:, rows, :], dep[:, rows, :]
        wet_u = (jnp.minimum(count, ring_e(count)) > 0.0).astype(jnp.float32)
        wet_v = (jnp.minimum(count, cnt[:, strip(r, 1), :]) > 0.0).astype(jnp.float32)
        mu[:, rows, :] = wet_u
        mv[:, rows, :] = wet_v
        au[:, rows, :] = wet_u * (0.25 * dt_fast * f_u)
        av[:, rows, :] = wet_v * (0.25 * dt_fast * f_v)
        bu[:, rows, :] = wet_u * (dt_fast * dt_fast) * fx[:, rows, :]
        bv[:, rows, :] = wet_v * (dt_fast * dt_fast) * fy[:, rows, :]
        scale = 0.5 * GRAVITY * dt_fast * dt_fast
        cu[:, rows, :] = wet_u * (scale * (depth + ring_e(depth)))
        cv[:, rows, :] = wet_v * (scale * (depth + dep[:, strip(r, 1), :]))
        ua[:, rows, :] = dt_fast * ua[:, rows, :]
        va[:, rows, :] = dt_fast * va[:, rows, :]
        accu[:, pl.ds(SL * r, SL), :] = jnp.zeros((NC, SL, LN), jnp.float32)
        accv[:, pl.ds(SL * r, SL), :] = jnp.zeros((NC, SL, LN), jnp.float32)

    def subcycle(n, u_old, v_old, u_new, v_new, span, first):
        weight = wts[n]
        weight_old = wts[jnp.maximum(n - 1, 0)]
        for r in span:
            rows = strip(r)
            u = u_old[:, rows, :]
            eta[:, rows, :] = eta[:, rows, :] - (u - ring_w(u) + v_old[:, rows, :] - v_old[:, strip(r, -1), :])
        for r in span:
            rows, rows_a = strip(r), pl.ds(SL * r, SL)
            u, v, e = u_old[:, rows, :], v_old[:, rows, :], eta[:, rows, :]
            w2 = v + v_old[:, strip(r, -1), :]
            y2 = u + u_old[:, strip(r, 1), :]
            ug, vg = (mu[:, rows, :] * u, mv[:, rows, :] * v) if first else (u, v)
            un = ug + (au[:, rows, :] * (w2 + ring_e(w2)) + bu[:, rows, :] - cu[:, rows, :] * (ring_e(e) - e))
            vn = vg + (bv[:, rows, :] - av[:, rows, :] * (y2 + ring_w(y2))
                       - cv[:, rows, :] * (eta[:, strip(r, 1), :] - e))
            u_new[:, rows, :] = un
            v_new[:, rows, :] = vn
            if u_new is ua:
                accu[:, rows_a, :] = accu[:, rows_a, :] + (weight_old * u[:NC] + weight * un[:NC])
                accv[:, rows_a, :] = accv[:, rows_a, :] + (weight_old * v[:NC] + weight * vn[:NC])

    def pair_of(pair, span, first):
        subcycle(2 * pair, ua, va, ubt, vbt, span, first)
        subcycle(2 * pair + 1, ubt, vbt, ua, va, span, False)

    pair_of(0, range(STRIPS), True)

    narrow = STRIPS - 2
    turning = (SL * (STRIPS - narrow) - 2) // 2

    @pl.loop(1, turning)
    def _(pair):
        pair_of(pair, range(STRIPS), False)

    @pl.when(row == 0)
    def _():
        @pl.loop(turning, LEVELS // 2)
        def _(pair):
            pair_of(pair, range(narrow), False)

    @pl.when(row == 1)
    def _():
        @pl.loop(turning, LEVELS // 2)
        def _(pair):
            pair_of(pair, range(STRIPS - narrow, STRIPS), False)

    @pl.loop(0, NR // SL)
    def _(r):
        eb = pl.multiple_of(own + SL * r, SL)
        rows = pl.ds(eb, SL)
        rows_a = pl.ds(pl.multiple_of(eb - PAD, SL), SL)
        out = pl.ds(pl.multiple_of(SL * r, SL), SL)
        depth = dep[:, rows, :]
        hu = 0.5 * (depth + ring_e(depth))[:NC]
        hv = 0.5 * (depth + dep[:, pl.ds(eb + 1, SL), :])[:NC]
        aux[3, :, out, :] = LEVELS / TIME_STEP * accu[:, rows_a, :] / hu - meanu[:, out, :]
        aux[4, :, out, :] = LEVELS / TIME_STEP * accv[:, rows_a, :] / hv - meanv[:, out, :]
        aux[5, :, out, :] = eta[0:NC, rows, :]
        aux[6, :, out, :] = (LEVELS / TIME_STEP) * ua[0:NC, rows, :]
        aux[7, :, out, :] = (LEVELS / TIME_STEP) * va[0:NC, rows, :]

    for copy in row_copies + flat_copies + x_copies + w_copies + late:
        copy.wait_send()


def finish_kernel(vu, vv, vt, vs, aux, o_eta, o_tu, o_tv, o_u, o_v, o_t, o_s, *scratch):
    flat_bufs, cube_bufs, sem_f, sem_c = scratch[:3], scratch[3:7], scratch[7], scratch[8]
    flat_copies = []
    for i, (buf, ref) in enumerate(zip(flat_bufs, (o_eta, o_tu, o_tv))):
        for c in range(NC):
            buf[:, pl.ds(c * LN, LN)] = aux[5 + i, c]
        flat_copies.append(pltpu.make_async_copy(buf, ref, sem_f.at[i]))

    def copies(r):
        rows = pl.ds(SL * r if isinstance(r, int) else pl.multiple_of(SL * r, SL), SL)
        return [pltpu.make_async_copy(buf.at[:, rows, :], ref.at[:, rows, :], sem_c.at[i, r])
                for i, (buf, ref) in enumerate(zip(cube_bufs, (o_u, o_v, o_t, o_s)))]

    @pl.loop(0, NR // SL)
    def _(r):
        finish_rows(pl.ds(pl.multiple_of(SL * r, SL), SL), vu, vv, vt, vs, aux, *cube_bufs)
        for copy in copies(r):
            copy.start()

    for copy in flat_copies:
        copy.start()
    for r in range(NR // SL):
        for copy in copies(r):
            copy.wait()
    for copy in flat_copies:
        copy.wait()


def finish_rows(rows, vu, vv, vt, vs, aux, o_u, o_v, o_t, o_s):
    def put(ref, value):
        for c in range(NC):
            ref[rows, pl.ds(c * LN, LN)] = value[c]

    count, lu, lv, gu, gv = (aux[i, :, rows, :] for i in range(5))
    xu = xv = xt = xs = on_u = on_v = inside = None
    for k in reversed(range(LEVELS)):
        level = float(k)
        wu, wv, xt_new, xs_new = (ref[k, :, rows, :] for ref in (vu, vv, vt, vs))
        if k == LEVELS - 1:
            xu, xv = END_V[k] * wu, END_V[k] * wv
        else:
            xu = jnp.where(on_u, wu + CARRY_V[k] * xu, END_V[k] * wu)
            xv = jnp.where(on_v, wv + CARRY_V[k] * xv, END_V[k] * wv)
            xt_new = xt_new + CARRY_D[k] * jnp.where(inside, xt, 0.0)
            xs_new = xs_new + CARRY_D[k] * jnp.where(inside, xs, 0.0)
        xt, xs = xt_new, xs_new
        on_u, on_v, inside = lu > level, lv > level, count > level
        put(o_u.at[k], jnp.where(on_u, xu + gu, 0.0))
        put(o_v.at[k], jnp.where(on_v, xv + gv, 0.0))
        put(o_t.at[k], xt)
        put(o_s.at[k], xs)


def solution(mesh):
    n_col = mesh.shape['col']

    def step(vel_u, vel_v, temperature, salinity, surf_eta, trans_u, trans_v, bottom_depth, level_count, avg_weights):
        f32 = jnp.float32
        swept = jax.ShapeDtypeStruct((LEVELS, NC, NR, LN), f32)
        vmem = pl.BlockSpec(memory_space=pltpu.VMEM)
        anywhere = pl.BlockSpec(memory_space=pl.ANY)
        wide = pltpu.VMEM((NC + 1, EROWS, LN), f32)
        cube = pltpu.VMEM((LEVELS, NC + 1, NR + 16, LN), f32)
        acc = pltpu.VMEM((NC, EXT, LN), f32)
        mean = pltpu.VMEM((NC, NR, LN), f32)
        dma = pltpu.SemaphoreType.DMA
        swept_all = pl.pallas_call(
            functools.partial(step_kernel, n_col),
            out_shape=(swept,) * 4 + (jax.ShapeDtypeStruct((SL, NC, NR, LN), f32),),
            in_specs=[anywhere] * 10,
            out_specs=(vmem,) * 5,
            scratch_shapes=[cube] * 4 + [wide] * 7 + [pltpu.VMEM((NC, EROWS, LN), jnp.int32)] + [wide] * 10
            + [acc, acc, mean, mean,
               *[pltpu.VMEM((2, rows, LN), f32) for rows in (NR, NR, EROWS, EROWS, NR, EROWS)],
               pltpu.SMEM((LEVELS,), f32), dma(()), dma((4, NC - 2, 2))]
            + [dma((4, NC)), dma((5, NC)), dma((4, NC)), dma((4, NC)), dma((5, NC)), dma((5, NC)),
               *[dma((2, 2))] * 6, dma((2,)), dma((2,))],
            compiler_params=pltpu.CompilerParams(
                collective_id=0, has_side_effects=True, vmem_limit_bytes=33 * 1024 * 1024),
            name='step_kernel',
        )(*[pltpu.with_memory_space_constraint(x, pltpu.HBM) for x in (avg_weights, vel_u, vel_v, temperature, salinity, surf_eta, trans_u, trans_v, bottom_depth, level_count)])
        flat_out = jax.ShapeDtypeStruct(surf_eta.shape, f32)
        cube_out = jax.ShapeDtypeStruct(vel_u.shape, f32)
        return pl.pallas_call(
            finish_kernel,
            out_shape=(flat_out,) * 3 + (cube_out,) * 4,
            in_specs=[vmem] * 5,
            out_specs=(anywhere,) * 7,
            scratch_shapes=[pltpu.VMEM(surf_eta.shape, f32)] * 3 + [pltpu.VMEM(vel_u.shape, f32)] * 4
            + [dma((3,)), dma((4, NR // SL))],
            compiler_params=pltpu.CompilerParams(vmem_limit_bytes=20 * 1024 * 1024),
            name='finish_kernel',
        )(*swept_all)

    cube = P(None, 'row', 'col')
    flat = P('row', 'col')
    return jax.shard_map(step, mesh=mesh, in_specs=(cube, cube, cube, cube, flat, flat, flat, flat, flat, P()), out_specs=(flat, flat, flat, cube, cube, cube, cube), check_vma=False)
```

```python
import functools

import jax
import jax.numpy as jnp
from jax import lax
from jax.experimental import pallas as pl
from jax.experimental.pallas import tpu as pltpu
from jax.sharding import PartitionSpec as P

TIME_STEP = 1.0
GRAVITY = 16.0
BC_GRAVITY = 4.0
EXPAND_T = 0.2
CONTRACT_S = 0.6
CORIO_F0 = 0.4
CORIO_BETA = 0.4
VISC_R = 2.0
DIFF_R = 0.5

MESH = pl.DeviceIdType.MESH
SL = 8
LN = 128
LEVELS = 30
NR = 64
NC = 4
HY = 32
HX = 32
EXT = NR + HY
PAD = SL
EROWS = EXT + 2 * PAD
STRIPS = EXT // SL
LANE_COUNT = 4 * LEVELS
LANE_DEPTH = LANE_COUNT + 1


def elimination(strength):
    pivots, ends = [], []
    for level in range(LEVELS):
        below = strength * strength / pivots[-1] if level else strength
        pivots.append(1.0 + 2.0 * strength - below)
        ends.append(1.0 + strength - below)
    inverse = [1.0 / pivot for pivot in pivots]
    carry = [strength / pivot for pivot in pivots]
    ending = [pivot / end for pivot, end in zip(pivots, ends)]
    return inverse, carry, ending


INV_V, CARRY_V, END_V = elimination(VISC_R)
INV_D, CARRY_D, END_D = elimination(DIFF_R)


def roll_e(x):
    return pltpu.roll(x, 127, x.ndim - 1)


def roll_w(x):
    return pltpu.roll(x, 1, x.ndim - 1)


def turn(x, amount):
    amount = amount % LN
    return pltpu.roll(x, amount, x.ndim - 1) if amount else x


def following(x):
    return jnp.concatenate([x[1:], x[:1]], axis=0)


def preceding(x):
    return jnp.concatenate([x[-1:], x[:-1]], axis=0)


def step_kernel(n_col, wts_h, u_h, v_h, t_h, s_h, eta_h, tu_h, tv_h, dep_h, cnt_h,
                vu, vv, vt, vs, aux,
                ub, vb, tb, sb, eta, ua, ubt, va, vbt, dep, cnt, cnt_i, fx, fy,
                au, av, bu, bv, cu, cv, mu, mv, accu, accv, meanu, meanv,
                pk, pkl, rx, rxl, pkw, rxw, wts, sem_w, sem_half,
                sem_in, sem_2d, sem_rs, sem_rr, sem_fs, sem_fr, sem_xs, sem_xr, sem_ls, sem_lr, sem_ws, sem_wr, sem_gs, sem_gr):
    col = lax.axis_index('col')
    row = lax.axis_index('row')
    east = lax.rem(col + 1, n_col)
    west = lax.rem(col + n_col - 1, n_col)
    other = 1 - row
    own = pl.multiple_of(PAD + HY * row, SL)
    near = pl.multiple_of(HY * other, SL)
    far = pl.multiple_of(PAD + NR * row, SL)
    mid = PAD + HY
    lane = lax.broadcasted_iota(jnp.int32, (SL, LN), 1)
    sub = lax.broadcasted_iota(jnp.int32, (SL, LN), 0)
    cubes = ((u_h, ub), (v_h, vb), (t_h, tb), (s_h, sb))
    flats = ((eta_h, eta), (tu_h, ua), (tv_h, va), (dep_h, dep), (cnt_h, cnt_i))

    loads = {}
    part = NR // 2
    for c in range(1, NC - 1):
        for f, (src, dst) in enumerate(cubes):
            for h in range(2):
                loads[f, c, h] = pltpu.make_async_copy(
                    src.at[:, pl.ds(part * h, part), pl.ds(c * LN, LN)],
                    dst.at[:, c, pl.ds(SL + part * h, part), :], sem_half.at[f, c - 1, h])
    for c in (0, NC - 1):
        for f, (src, dst) in enumerate(cubes):
            loads[f, c] = pltpu.make_async_copy(
                src.at[:, :, pl.ds(c * LN, LN)], dst.at[:, c, pl.ds(SL, NR), :], sem_in.at[f, c])
    flat_loads = []
    for f, (src, dst) in enumerate(flats):
        for c in range(NC):
            flat_loads.append(pltpu.make_async_copy(
                src.at[:, pl.ds(c * LN, LN)], dst.at[c, pl.ds(own, NR), :], sem_2d.at[f, c]))
    for c in (0, 3):
        for f in range(4):
            loads[f, c].start()
    for copy in flat_loads:
        copy.start()
    for h in range(2):
        for f in range(len(cubes)):
            for c in range(1, NC - 1):
                loads[f, c, h].start()
    weight_load = pltpu.make_async_copy(wts_h, wts, sem_w)
    weight_load.start()

    barrier = pltpu.get_barrier_semaphore()
    for peer in ({'col': east, 'row': row}, {'col': west, 'row': row}, {'col': col, 'row': other},
                 {'col': east, 'row': other}, {'col': west, 'row': other}):
        pl.semaphore_signal(barrier, inc=1, device_id=peer, device_id_type=MESH)

    wall = pl.multiple_of((NR + SL) * row, SL)
    zero4 = jnp.zeros((NC, SL, LN), jnp.float32)

    @pl.loop(0, LEVELS)
    def _(k):
        for _, dst in cubes:
            dst[k, 0:NC, pl.ds(wall, SL), :] = zero4

    zero5 = jnp.zeros((NC + 1, SL, LN), jnp.float32)
    for start in (0, PAD + EXT):
        for ref in (eta, ua, ubt, va, vbt, dep, cnt, fx, fy):
            ref[:, pl.ds(start, SL), :] = zero5
        cnt_i[:, pl.ds(start, SL), :] = jnp.zeros((NC, SL, LN), jnp.int32)
        rx[:, pl.ds(start, SL), :] = jnp.zeros((2, SL, LN), jnp.float32)

    pl.semaphore_wait(barrier, 5)

    row_copies = []
    edge_src = pl.multiple_of((NR - SL) * other, SL)
    for f, (src, dst) in enumerate(cubes):
        for c in range(NC):
            row_copies.append(pltpu.make_async_remote_copy(
                src_ref=src.at[:, pl.ds((NR - 1) * other, 1), pl.ds(c * LN, LN)],
                dst_ref=dst.at[:, c, pl.ds((NR + SL) * row + (SL - 1) * other, 1), :],
                send_sem=sem_rs.at[f, c], recv_sem=sem_rr.at[f, c],
                device_id={'col': col, 'row': other}, device_id_type=MESH))
    flat_copies = []
    for f, (src, dst) in enumerate(flats):
        for c in range(NC):
            flat_copies.append(pltpu.make_async_remote_copy(
                src_ref=src.at[pl.ds(near, HY), pl.ds(c * LN, LN)],
                dst_ref=dst.at[c, pl.ds(far, HY), :],
                send_sem=sem_fs.at[f, c], recv_sem=sem_fr.at[f, c],
                device_id={'col': col, 'row': other}, device_id_type=MESH))
    for copy in row_copies + flat_copies:
        copy.start()

    groups = (NR // SL, SL, LN)
    lanes = lax.broadcasted_iota(jnp.int32, (1, SL, LN), 2)
    acc_e = acc_w = jnp.zeros(groups, jnp.float32)
    for f, (_, buf) in enumerate(cubes):
        loads[f, 0].wait()
        loads[f, NC - 1].wait()
        for k in range(LEVELS):
            m = f * LEVELS + k
            both = jnp.where(lanes == LN - 1, buf[k, NC - 1, pl.ds(SL, NR), :].reshape(groups),
                             buf[k, 0, pl.ds(SL, NR), :].reshape(groups))
            both = turn(both, m)
            acc_e = jnp.where(lanes == (m - 1) % LN, both, acc_e)
            acc_w = jnp.where(lanes == m, both, acc_w)
    for copy in flat_loads:
        copy.wait()
    for m, ref in ((LANE_COUNT, cnt_i), (LANE_DEPTH, dep)):
        last = ref[NC - 1, pl.ds(own, NR), :].astype(jnp.float32).reshape(groups)
        first = ref[0, pl.ds(own, NR), :].astype(jnp.float32).reshape(groups)
        acc_e = jnp.where(lanes == m - 1, turn(last, m), acc_e)
        acc_w = jnp.where(lanes == m, turn(first, m), acc_w)
    pk[0] = acc_e.reshape(NR, LN)
    pk[1] = acc_w.reshape(NR, LN)

    def side_by_side(dst, refs):
        for r in range(NR // SL):
            rows_e = pl.ds(pl.multiple_of(own + SL * r, SL), SL)
            acc_e = turn(refs[0][NC - 1, rows_e, :], HX)
            acc_w = refs[0][0, rows_e, :]
            for p, ref in enumerate(refs[1:], 1):
                here = lane >= p * HX
                acc_e = jnp.where(here, turn(ref[NC - 1, rows_e, :], HX * (p + 1)), acc_e)
                acc_w = jnp.where(here, turn(ref[0, rows_e, :], HX * p), acc_w)
            dst[0, pl.ds(SL * r, SL), :] = acc_e
            dst[1, pl.ds(SL * r, SL), :] = acc_w

    def sideways(src, dst, sends, recvs, from_row, to_row, rows):
        copies = []
        for d, side in enumerate((east, west)):
            copies.append(pltpu.make_async_remote_copy(
                src_ref=src.at[d], dst_ref=dst.at[d, pl.ds(own, NR), :],
                send_sem=sends.at[d, 0], recv_sem=recvs.at[d, 0],
                device_id={'col': side, 'row': row}, device_id_type=MESH))
            copies.append(pltpu.make_async_remote_copy(
                src_ref=src.at[d, pl.ds(from_row, rows), :], dst_ref=dst.at[d, pl.ds(to_row, rows), :],
                send_sem=sends.at[d, 1], recv_sem=recvs.at[d, 1],
                device_id={'col': side, 'row': other}, device_id_type=MESH))
        return copies

    corner = pl.multiple_of(PAD + HY - SL + (NR - HY + SL) * row, SL)
    x_copies = sideways(pk, rx, sem_xs, sem_xr, edge_src, corner, SL)
    for copy in x_copies:
        copy.start()
    side_by_side(pkw, (eta, ua, va, dep))

    for copy in flat_copies:
        copy.wait_recv()
    for r in range(STRIPS):
        cnt[0:NC, pl.ds(PAD + SL * r, SL), :] = cnt_i[:, pl.ds(PAD + SL * r, SL), :].astype(jnp.float32)


    def inner_half(h):
        for c in range(1, NC - 1):
            for f in range(len(cubes)):
                loads[f, c, h].wait()

    inner_half(0)
    w_copies = sideways(pkw, rxw, sem_ws, sem_wr, near, far, HY)
    for copy in w_copies:
        copy.start()
    for copy in row_copies:
        copy.wait_recv()

    half = 0.5 * BC_GRAVITY / LEVELS
    first0 = lax.broadcasted_iota(jnp.int32, (1, SL, LN), 2) == 0
    last127 = lax.broadcasted_iota(jnp.int32, (1, SL, LN), 2) == 127

    def shift_e(mine, following_tile):
        return roll_e(jnp.where(first0, following_tile, mine))

    def shift_w(mine, preceding_tile):
        return roll_w(jnp.where(last127, preceding_tile, mine))

    def ring_e(x):
        return shift_e(x, following(x))

    def ring_w(x):
        return shift_w(x, preceding(x))

    def inner(x):
        return x[1:3], x[2:4], x[0:2]

    def outer(x):
        return (jnp.concatenate([x[0:1], x[3:4]], axis=0), jnp.concatenate([x[1:2], x[4:5]], axis=0),
                jnp.concatenate([x[4:5], x[2:3]], axis=0))

    def every(x):
        return x[0:4], x[1:5], jnp.concatenate([x[4:5], x[0:3]], axis=0)

    def momentum(r, tiles, places):
        rb = pl.multiple_of(SL + SL * r, SL)
        eb = pl.multiple_of(own + SL * r, SL)
        out = pl.ds(pl.multiple_of(SL * r, SL), SL)
        y = (NR * row + SL * r + sub).astype(jnp.float32)
        fu4 = 0.25 * (CORIO_F0 + CORIO_BETA * ((y + 0.5) / (2 * NR) - 0.5))
        fv4 = 0.25 * (CORIO_F0 + CORIO_BETA * ((y + 1.0) / (2 * NR) - 0.5))

        def load(ref, k, dr=0):
            return ref[k, :, pl.ds(rb + dr, SL), :]

        def put(ref, rows, value):
            for i, c in enumerate(places):
                ref[c, rows, :] = value[i]

        count, count_e, _ = tiles(cnt[:, pl.ds(eb, SL), :])
        lu = jnp.minimum(count, shift_e(count, count_e))
        lv = jnp.minimum(count, tiles(cnt[:, pl.ds(eb + 1, SL), :])[0])
        qx = qy = su = sv = sdu = sdv = jnp.zeros((len(places), SL, LN), jnp.float32)
        wu = wv = None
        for k in range(LEVELS):
            u, ue, uw = tiles(load(ub, k))
            un, _, unw = tiles(load(ub, k, 1))
            us = tiles(load(ub, k, -1))[0]
            v, ve, vw = tiles(load(vb, k))
            vn = tiles(load(vb, k, 1))[0]
            vso, vse, _ = tiles(load(vb, k, -1))
            s0, s_e, _ = tiles(load(sb, k))
            t0, t_e, _ = tiles(load(tb, k))
            rho = (CONTRACT_S * half) * s0 - (EXPAND_T * half) * t0
            rho_e = (CONTRACT_S * half) * s_e - (EXPAND_T * half) * t_e
            rho_n = (CONTRACT_S * half) * tiles(load(sb, k, 1))[0] - (EXPAND_T * half) * tiles(load(tb, k, 1))[0]
            w2 = v + vso
            w4 = w2 + shift_e(w2, ve + vse)
            y2 = u + un
            y4 = y2 + shift_w(y2, uw + unw)
            dx = shift_e(rho, rho_e) - rho
            dy = rho_n - rho
            px = qx + dx
            qx = px + dx
            py = qy + dy
            qy = py + dy
            du = w4 * (fu4 - 0.125 * (un - us)) - (0.5 * u) * (shift_e(u, ue) - shift_w(u, uw)) - px
            dv = -(y4 * (fv4 + 0.125 * (shift_e(v, ve) - shift_w(v, vw))) + (0.5 * v) * (vn - vso) + py)
            on_u = lu > float(k)
            on_v = lv > float(k)
            su = su + jnp.where(on_u, u, 0.0)
            sv = sv + jnp.where(on_v, v, 0.0)
            sdu = sdu + jnp.where(on_u, du, 0.0)
            sdv = sdv + jnp.where(on_v, dv, 0.0)
            tu, tv = u + du, v + dv
            wu = INV_V[k] * (tu if k == 0 else tu + VISC_R * wu)
            wv = INV_V[k] * (tv if k == 0 else tv + VISC_R * wv)
            put(vu.at[k], out, wu)
            put(vv.at[k], out, wv)
        inv_u = 1.0 / jnp.maximum(lu, 1.0)
        inv_v = 1.0 / jnp.maximum(lv, 1.0)
        depth, depth_e, _ = tiles(dep[:, pl.ds(eb, SL), :])
        hu = 0.5 * (depth + shift_e(depth, depth_e))
        hv = 0.5 * (depth + tiles(dep[:, pl.ds(eb + 1, SL), :])[0])
        put(fx, pl.ds(eb, SL), hu * (sdu * inv_u) / TIME_STEP)
        put(fy, pl.ds(eb, SL), hv * (sdv * inv_v) / TIME_STEP)
        put(meanu, out, (su + sdu) * inv_u)
        put(meanv, out, (sv + sdv) * inv_v)
        put(aux.at[0], out, count)
        put(aux.at[1], out, lu)
        put(aux.at[2], out, lv)

    def tracers(r):
        rb = pl.multiple_of(SL + SL * r, SL)
        eb = pl.multiple_of(own + SL * r, SL)
        out = pl.ds(pl.multiple_of(SL * r, SL), SL)

        def load(ref, k, dr=0):
            return ref[k, :, pl.ds(rb + dr, SL), :]

        count = cnt[:, pl.ds(eb, SL), :]
        lu = jnp.minimum(count, ring_e(count))
        count = count[:NC]
        lv = jnp.minimum(count, cnt[0:NC, pl.ds(eb + 1, SL), :])
        lvs = jnp.minimum(count, cnt[0:NC, pl.ds(eb - 1, SL), :])
        carried = [None, None]
        inside = count > 0.0
        for k in range(LEVELS):
            level = float(k)
            ge = TIME_STEP * jnp.where(lu > level, load(ub, k), 0.0)
            ge, _, gw = every(ge)
            gw = shift_w(ge, gw)
            gn = TIME_STEP * jnp.where(lv > level, load(vb, k)[:NC], 0.0)
            gs = TIME_STEP * jnp.where(lvs > level, load(vb, k, -1)[:NC], 0.0)
            keep = 2.0 - (ge - gw + gn - gs)
            inside_next = count > level + 1.0
            ending = 0.5 * INV_D[k] * END_D[k]
            pivot = ending if k == LEVELS - 1 else jnp.where(inside_next, 0.5 * INV_D[k], ending)
            for i, (buf, dst) in enumerate(((tb, vt), (sb, vs))):
                q, qe, qw = every(load(buf, k))
                twice = keep * q - (ge * shift_e(q, qe) - gw * shift_w(q, qw)
                                    + gn * load(buf, k, 1)[:NC] - gs * load(buf, k, -1)[:NC])
                w = pivot * (twice if k == 0 else twice + 2.0 * DIFF_R * carried[i])
                carried[i] = w
                dst[k, :, out, :] = jnp.where(inside, w, q)
            inside = inside_next

    @pl.loop(0, NR // SL)
    def _(r):
        @pl.when(r == part // SL - 1)
        def _():
            inner_half(1)

        momentum(r, inner, (1, 2))

    for copy in x_copies:
        copy.wait_recv()

    def unpack(rows, shape):
        even = lax.rem(lanes if len(shape) == 3 else lane, 2) == 0
        from_west, from_east = rx[0, rows, :].reshape(shape), rx[1, rows, :].reshape(shape)
        return jnp.where(even, from_east, from_west), jnp.where(even, from_west, from_east)

    def unpack_cube(f, rows, merged):
        for k in range(LEVELS):
            m = f * LEVELS + k
            cubes[f][1][k, NC, rows, :] = turn(merged[m % 2], -m).reshape(rows.size, LN)

    merged = unpack(pl.ds(own, NR), groups)
    for f in range(len(cubes)):
        unpack_cube(f, pl.ds(SL, NR), merged)
    cnt[NC, pl.ds(own, NR), :] = turn(merged[LANE_COUNT % 2], -LANE_COUNT).reshape(NR, LN)
    dep[NC, pl.ds(own, NR), :] = turn(merged[LANE_DEPTH % 2], -LANE_DEPTH).reshape(NR, LN)
    unpack_cube(1, pl.ds(0, SL), unpack(pl.ds(pl.multiple_of(own - SL, SL), SL), (SL, LN)))
    unpack_cube(0, pl.ds(SL + NR, SL), unpack(pl.ds(pl.multiple_of(own + NR, SL), SL), (SL, LN)))

    @pl.loop(0, NR // SL)
    def _(r):
        momentum(r, outer, (0, 3))

    side_by_side(pkl, (fx, fy, cnt))

    late = []
    for f, ref in enumerate((fx, fy)):
        late.append(pltpu.make_async_remote_copy(
            src_ref=ref.at[pl.ds(0, NC), pl.ds(mid, HY), :], dst_ref=ref.at[pl.ds(0, NC), pl.ds(far, HY), :],
            send_sem=sem_gs.at[f], recv_sem=sem_gr.at[f],
            device_id={'col': col, 'row': other}, device_id_type=MESH))
    late += sideways(pkl, rxl, sem_ls, sem_lr, near, far, HY)
    for copy in late:
        copy.start()

    @pl.loop(0, NR // SL)
    def _(r):
        tracers(r)

    for copy in w_copies + late:
        copy.wait_recv()
    weight_load.wait()

    def strip(r, dr=0):
        return pl.ds(PAD + SL * r + dr, SL)

    for r in range(STRIPS):
        for p, ref, src in ((0, eta, 1), (1, ua, 1), (2, va, 1), (3, dep, 1), (0, fx, 2), (1, fy, 2), (2, cnt, 2)):
            from_east = rxw[1, strip(r), :] if src == 1 else rxl[1, strip(r), :]
            from_west = rxw[0, strip(r), :] if src == 1 else rxl[0, strip(r), :]
            ref[NC, strip(r), :] = jnp.where(
                lane < HX, turn(from_east, -HX * p),
                jnp.where(lane >= LN - HX, turn(from_west, LN - HX - HX * p), 0.0))

    dt_fast = TIME_STEP / LEVELS
    for r in range(STRIPS):
        y = (HY * row + SL * r + sub).astype(jnp.float32)
        f_u = CORIO_F0 + CORIO_BETA * ((y + 0.5) / (2 * NR) - 0.5)
        f_v = CORIO_F0 + CORIO_BETA * ((y + 1.0) / (2 * NR) - 0.5)
        rows = strip(r)
        count, depth = cnt[:, rows, :], dep[:, rows, :]
        wet_u = (jnp.minimum(count, ring_e(count)) > 0.0).astype(jnp.float32)
        wet_v = (jnp.minimum(count, cnt[:, strip(r, 1), :]) > 0.0).astype(jnp.float32)
        mu[:, rows, :] = wet_u
        mv[:, rows, :] = wet_v
        au[:, rows, :] = wet_u * (0.25 * dt_fast * f_u)
        av[:, rows, :] = wet_v * (0.25 * dt_fast * f_v)
        bu[:, rows, :] = wet_u * (dt_fast * dt_fast) * fx[:, rows, :]
        bv[:, rows, :] = wet_v * (dt_fast * dt_fast) * fy[:, rows, :]
        scale = 0.5 * GRAVITY * dt_fast * dt_fast
        cu[:, rows, :] = wet_u * (scale * (depth + ring_e(depth)))
        cv[:, rows, :] = wet_v * (scale * (depth + dep[:, strip(r, 1), :]))
        ua[:, rows, :] = dt_fast * ua[:, rows, :]
        va[:, rows, :] = dt_fast * va[:, rows, :]
        accu[:, pl.ds(SL * r, SL), :] = jnp.zeros((NC, SL, LN), jnp.float32)
        accv[:, pl.ds(SL * r, SL), :] = jnp.zeros((NC, SL, LN), jnp.float32)

    def subcycle(n, u_old, v_old, u_new, v_new, span, first):
        weight = wts[n]
        weight_old = wts[jnp.maximum(n - 1, 0)]
        for r in span:
            rows = strip(r)
            u = u_old[:, rows, :]
            eta[:, rows, :] = eta[:, rows, :] - (u - ring_w(u) + v_old[:, rows, :] - v_old[:, strip(r, -1), :])
        for r in span:
            rows, rows_a = strip(r), pl.ds(SL * r, SL)
            u, v, e = u_old[:, rows, :], v_old[:, rows, :], eta[:, rows, :]
            w2 = v + v_old[:, strip(r, -1), :]
            y2 = u + u_old[:, strip(r, 1), :]
            ug, vg = (mu[:, rows, :] * u, mv[:, rows, :] * v) if first else (u, v)
            un = ug + (au[:, rows, :] * (w2 + ring_e(w2)) + bu[:, rows, :] - cu[:, rows, :] * (ring_e(e) - e))
            vn = vg + (bv[:, rows, :] - av[:, rows, :] * (y2 + ring_w(y2))
                       - cv[:, rows, :] * (eta[:, strip(r, 1), :] - e))
            u_new[:, rows, :] = un
            v_new[:, rows, :] = vn
            if u_new is ua:
                accu[:, rows_a, :] = accu[:, rows_a, :] + (weight_old * u[:NC] + weight * un[:NC])
                accv[:, rows_a, :] = accv[:, rows_a, :] + (weight_old * v[:NC] + weight * vn[:NC])

    def pair_of(pair, span, first):
        subcycle(2 * pair, ua, va, ubt, vbt, span, first)
        subcycle(2 * pair + 1, ubt, vbt, ua, va, span, False)

    pair_of(0, range(STRIPS), True)

    narrow = STRIPS - 2
    turning = (SL * (STRIPS - narrow) - 2) // 2

    @pl.loop(1, turning)
    def _(pair):
        pair_of(pair, range(STRIPS), False)

    @pl.when(row == 0)
    def _():
        @pl.loop(turning, LEVELS // 2)
        def _(pair):
            pair_of(pair, range(narrow), False)

    @pl.when(row == 1)
    def _():
        @pl.loop(turning, LEVELS // 2)
        def _(pair):
            pair_of(pair, range(STRIPS - narrow, STRIPS), False)

    @pl.loop(0, NR // SL)
    def _(r):
        eb = pl.multiple_of(own + SL * r, SL)
        rows = pl.ds(eb, SL)
        rows_a = pl.ds(pl.multiple_of(eb - PAD, SL), SL)
        out = pl.ds(pl.multiple_of(SL * r, SL), SL)
        depth = dep[:, rows, :]
        hu = 0.5 * (depth + ring_e(depth))[:NC]
        hv = 0.5 * (depth + dep[:, pl.ds(eb + 1, SL), :])[:NC]
        aux[3, :, out, :] = LEVELS / TIME_STEP * accu[:, rows_a, :] / hu - meanu[:, out, :]
        aux[4, :, out, :] = LEVELS / TIME_STEP * accv[:, rows_a, :] / hv - meanv[:, out, :]
        aux[5, :, out, :] = eta[0:NC, rows, :]
        aux[6, :, out, :] = (LEVELS / TIME_STEP) * ua[0:NC, rows, :]
        aux[7, :, out, :] = (LEVELS / TIME_STEP) * va[0:NC, rows, :]

    for copy in row_copies + flat_copies + x_copies + w_copies + late:
        copy.wait_send()


def finish_kernel(vu, vv, vt, vs, aux, o_eta, o_tu, o_tv, o_u, o_v, o_t, o_s, *scratch):
    flat_bufs, cube_bufs, sem_f, sem_c = scratch[:3], scratch[3:7], scratch[7], scratch[8]
    flat_copies = []
    for i, (buf, ref) in enumerate(zip(flat_bufs, (o_eta, o_tu, o_tv))):
        for c in range(NC):
            buf[:, pl.ds(c * LN, LN)] = aux[5 + i, c]
        flat_copies.append(pltpu.make_async_copy(buf, ref, sem_f.at[i]))

    def copies(r):
        rows = pl.ds(SL * r if isinstance(r, int) else pl.multiple_of(SL * r, SL), SL)
        return [pltpu.make_async_copy(buf.at[:, rows, :], ref.at[:, rows, :], sem_c.at[i, r])
                for i, (buf, ref) in enumerate(zip(cube_bufs, (o_u, o_v, o_t, o_s)))]

    @pl.loop(0, NR // SL)
    def _(r):
        finish_rows(pl.ds(pl.multiple_of(SL * r, SL), SL), vu, vv, vt, vs, aux, *cube_bufs)
        for copy in copies(r):
            copy.start()

    for copy in flat_copies:
        copy.start()
    for r in range(NR // SL):
        for copy in copies(r):
            copy.wait()
    for copy in flat_copies:
        copy.wait()


def finish_rows(rows, vu, vv, vt, vs, aux, o_u, o_v, o_t, o_s):
    def put(ref, value):
        for c in range(NC):
            ref[rows, pl.ds(c * LN, LN)] = value[c]

    count, lu, lv, gu, gv = (aux[i, :, rows, :] for i in range(5))
    xu = xv = xt = xs = on_u = on_v = inside = None
    for k in reversed(range(LEVELS)):
        level = float(k)
        wu, wv, xt_new, xs_new = (ref[k, :, rows, :] for ref in (vu, vv, vt, vs))
        if k == LEVELS - 1:
            xu, xv = END_V[k] * wu, END_V[k] * wv
        else:
            xu = jnp.where(on_u, wu + CARRY_V[k] * xu, END_V[k] * wu)
            xv = jnp.where(on_v, wv + CARRY_V[k] * xv, END_V[k] * wv)
            xt_new = xt_new + CARRY_D[k] * jnp.where(inside, xt, 0.0)
            xs_new = xs_new + CARRY_D[k] * jnp.where(inside, xs, 0.0)
        xt, xs = xt_new, xs_new
        on_u, on_v, inside = lu > level, lv > level, count > level
        put(o_u.at[k], jnp.where(on_u, xu + gu, 0.0))
        put(o_v.at[k], jnp.where(on_v, xv + gv, 0.0))
        put(o_t.at[k], xt)
        put(o_s.at[k], xs)


def solution(mesh):
    n_col = mesh.shape['col']

    def step(vel_u, vel_v, temperature, salinity, surf_eta, trans_u, trans_v, bottom_depth, level_count, avg_weights):
        f32 = jnp.float32
        swept = jax.ShapeDtypeStruct((LEVELS, NC, NR, LN), f32)
        vmem = pl.BlockSpec(memory_space=pltpu.VMEM)
        anywhere = pl.BlockSpec(memory_space=pl.ANY)
        wide = pltpu.VMEM((NC + 1, EROWS, LN), f32)
        cube = pltpu.VMEM((LEVELS, NC + 1, NR + 16, LN), f32)
        acc = pltpu.VMEM((NC, EXT, LN), f32)
        mean = pltpu.VMEM((NC, NR, LN), f32)
        dma = pltpu.SemaphoreType.DMA
        swept_all = pl.pallas_call(
            functools.partial(step_kernel, n_col),
            out_shape=(swept,) * 4 + (jax.ShapeDtypeStruct((SL, NC, NR, LN), f32),),
            in_specs=[anywhere] * 10,
            out_specs=(vmem,) * 5,
            scratch_shapes=[cube] * 4 + [wide] * 7 + [pltpu.VMEM((NC, EROWS, LN), jnp.int32)] + [wide] * 10
            + [acc, acc, mean, mean,
               *[pltpu.VMEM((2, rows, LN), f32) for rows in (NR, NR, EROWS, EROWS, NR, EROWS)],
               pltpu.SMEM((LEVELS,), f32), dma(()), dma((4, NC - 2, 2))]
            + [dma((4, NC)), dma((5, NC)), dma((4, NC)), dma((4, NC)), dma((5, NC)), dma((5, NC)),
               *[dma((2, 2))] * 6, dma((2,)), dma((2,))],
            compiler_params=pltpu.CompilerParams(
                collective_id=0, has_side_effects=True, vmem_limit_bytes=33 * 1024 * 1024),
            name='step_kernel',
        )(*[pltpu.with_memory_space_constraint(x, pltpu.HBM) for x in (avg_weights, vel_u, vel_v, temperature, salinity, surf_eta, trans_u, trans_v, bottom_depth, level_count)])
        flat_out = jax.ShapeDtypeStruct(surf_eta.shape, f32)
        cube_out = jax.ShapeDtypeStruct(vel_u.shape, f32)
        return pl.pallas_call(
            finish_kernel,
            out_shape=(flat_out,) * 3 + (cube_out,) * 4,
            in_specs=[vmem] * 5,
            out_specs=(anywhere,) * 7,
            scratch_shapes=[pltpu.VMEM(surf_eta.shape, f32)] * 3 + [pltpu.VMEM(vel_u.shape, f32)] * 4
            + [dma((3,)), dma((4, NR // SL))],
            compiler_params=pltpu.CompilerParams(vmem_limit_bytes=20 * 1024 * 1024),
            name='finish_kernel',
        )(*swept_all)

    cube = P(None, 'row', 'col')
    flat = P('row', 'col')
    return jax.shard_map(step, mesh=mesh, in_specs=(cube, cube, cube, cube, flat, flat, flat, flat, flat, P()), out_specs=(flat, flat, flat, cube, cube, cube, cube), check_vma=False)
```

```python
import functools

import jax
import jax.numpy as jnp
from jax import lax
from jax.experimental import pallas as pl
from jax.experimental.pallas import tpu as pltpu
from jax.sharding import PartitionSpec as P

TIME_STEP = 1.0
GRAVITY = 16.0
BC_GRAVITY = 4.0
EXPAND_T = 0.2
CONTRACT_S = 0.6
CORIO_F0 = 0.4
CORIO_BETA = 0.4
VISC_R = 2.0
DIFF_R = 0.5

MESH = pl.DeviceIdType.MESH
SL = 8
LN = 128
LEVELS = 30
NR = 64
NC = 4
HY = 32
HX = 32
EXT = NR + HY
PAD = SL
EROWS = EXT + 2 * PAD
STRIPS = EXT // SL
LANE_COUNT = 4 * LEVELS
LANE_DEPTH = LANE_COUNT + 1


def elimination(strength):
    pivots, ends = [], []
    for level in range(LEVELS):
        below = strength * strength / pivots[-1] if level else strength
        pivots.append(1.0 + 2.0 * strength - below)
        ends.append(1.0 + strength - below)
    inverse = [1.0 / pivot for pivot in pivots]
    carry = [strength / pivot for pivot in pivots]
    ending = [pivot / end for pivot, end in zip(pivots, ends)]
    return inverse, carry, ending


INV_V, CARRY_V, END_V = elimination(VISC_R)
INV_D, CARRY_D, END_D = elimination(DIFF_R)


def roll_e(x):
    return pltpu.roll(x, 127, x.ndim - 1)


def roll_w(x):
    return pltpu.roll(x, 1, x.ndim - 1)


def turn(x, amount):
    amount = amount % LN
    return pltpu.roll(x, amount, x.ndim - 1) if amount else x


def following(x):
    return jnp.concatenate([x[1:], x[:1]], axis=0)


def preceding(x):
    return jnp.concatenate([x[-1:], x[:-1]], axis=0)


def step_kernel(n_col, wts_h, u_h, v_h, t_h, s_h, eta_h, tu_h, tv_h, dep_h, cnt_h,
                vu, vv, vt, vs, aux,
                ub, vb, tb, sb, eta, ua, ubt, va, vbt, dep, cnt, cnt_i, fx, fy,
                au, av, bu, bv, cu, cv, mu, mv, accu, accv, meanu, meanv,
                pk, pkl, rx, rxl, pkw, rxw, wts, sem_w, sem_half,
                sem_in, sem_2d, sem_rs, sem_rr, sem_fs, sem_fr, sem_xs, sem_xr, sem_ls, sem_lr, sem_ws, sem_wr, sem_gs, sem_gr):
    col = lax.axis_index('col')
    row = lax.axis_index('row')
    east = lax.rem(col + 1, n_col)
    west = lax.rem(col + n_col - 1, n_col)
    other = 1 - row
    own = pl.multiple_of(PAD + HY * row, SL)
    near = pl.multiple_of(HY * other, SL)
    far = pl.multiple_of(PAD + NR * row, SL)
    mid = PAD + HY
    lane = lax.broadcasted_iota(jnp.int32, (SL, LN), 1)
    sub = lax.broadcasted_iota(jnp.int32, (SL, LN), 0)
    cubes = ((u_h, ub), (v_h, vb), (t_h, tb), (s_h, sb))
    flats = ((eta_h, eta), (tu_h, ua), (tv_h, va), (dep_h, dep), (cnt_h, cnt_i))

    loads = {}
    part = NR // 2
    for c in range(1, NC - 1):
        for f, (src, dst) in enumerate(cubes):
            for h in range(2):
                loads[f, c, h] = pltpu.make_async_copy(
                    src.at[:, pl.ds(part * h, part), pl.ds(c * LN, LN)],
                    dst.at[:, c, pl.ds(SL + part * h, part), :], sem_half.at[f, c - 1, h])
    for c in (0, NC - 1):
        for f, (src, dst) in enumerate(cubes):
            loads[f, c] = pltpu.make_async_copy(
                src.at[:, :, pl.ds(c * LN, LN)], dst.at[:, c, pl.ds(SL, NR), :], sem_in.at[f, c])
    flat_loads = []
    for f, (src, dst) in enumerate(flats):
        for c in range(NC):
            flat_loads.append(pltpu.make_async_copy(
                src.at[:, pl.ds(c * LN, LN)], dst.at[c, pl.ds(own, NR), :], sem_2d.at[f, c]))
    for c in (0, 3):
        for f in range(4):
            loads[f, c].start()
    for copy in flat_loads:
        copy.start()
    for h in range(2):
        for f in range(len(cubes)):
            for c in range(1, NC - 1):
                loads[f, c, h].start()
    weight_load = pltpu.make_async_copy(wts_h, wts, sem_w)
    weight_load.start()

    barrier = pltpu.get_barrier_semaphore()
    for peer in ({'col': east, 'row': row}, {'col': west, 'row': row}, {'col': col, 'row': other},
                 {'col': east, 'row': other}, {'col': west, 'row': other}):
        pl.semaphore_signal(barrier, inc=1, device_id=peer, device_id_type=MESH)

    wall = pl.multiple_of((NR + SL) * row, SL)
    zero4 = jnp.zeros((NC, SL, LN), jnp.float32)

    @pl.loop(0, LEVELS)
    def _(k):
        for _, dst in cubes:
            dst[k, 0:NC, pl.ds(wall, SL), :] = zero4

    zero5 = jnp.zeros((NC + 1, SL, LN), jnp.float32)
    for start in (0, PAD + EXT):
        for ref in (eta, ua, ubt, va, vbt, dep, cnt, fx, fy):
            ref[:, pl.ds(start, SL), :] = zero5
        cnt_i[:, pl.ds(start, SL), :] = jnp.zeros((NC, SL, LN), jnp.int32)
        rx[:, pl.ds(start, SL), :] = jnp.zeros((2, SL, LN), jnp.float32)

    pl.semaphore_wait(barrier, 5)

    row_copies = []
    edge_src = pl.multiple_of((NR - SL) * other, SL)
    for f, (src, dst) in enumerate(cubes):
        for c in range(NC):
            row_copies.append(pltpu.make_async_remote_copy(
                src_ref=src.at[:, pl.ds((NR - 1) * other, 1), pl.ds(c * LN, LN)],
                dst_ref=dst.at[:, c, pl.ds((NR + SL) * row + (SL - 1) * other, 1), :],
                send_sem=sem_rs.at[f, c], recv_sem=sem_rr.at[f, c],
                device_id={'col': col, 'row': other}, device_id_type=MESH))
    flat_copies = []
    for f, (src, dst) in enumerate(flats):
        for c in range(NC):
            flat_copies.append(pltpu.make_async_remote_copy(
                src_ref=src.at[pl.ds(near, HY), pl.ds(c * LN, LN)],
                dst_ref=dst.at[c, pl.ds(far, HY), :],
                send_sem=sem_fs.at[f, c], recv_sem=sem_fr.at[f, c],
                device_id={'col': col, 'row': other}, device_id_type=MESH))
    for copy in row_copies + flat_copies:
        copy.start()

    groups = (NR // SL, SL, LN)
    lanes = lax.broadcasted_iota(jnp.int32, (1, SL, LN), 2)
    acc_e = acc_w = jnp.zeros(groups, jnp.float32)
    for f, (_, buf) in enumerate(cubes):
        loads[f, 0].wait()
        loads[f, NC - 1].wait()
        for k in range(LEVELS):
            m = f * LEVELS + k
            both = jnp.where(lanes == LN - 1, buf[k, NC - 1, pl.ds(SL, NR), :].reshape(groups),
                             buf[k, 0, pl.ds(SL, NR), :].reshape(groups))
            both = turn(both, m)
            acc_e = jnp.where(lanes == (m - 1) % LN, both, acc_e)
            acc_w = jnp.where(lanes == m, both, acc_w)
    for copy in flat_loads:
        copy.wait()
    for m, ref in ((LANE_COUNT, cnt_i), (LANE_DEPTH, dep)):
        last = ref[NC - 1, pl.ds(own, NR), :].astype(jnp.float32).reshape(groups)
        first = ref[0, pl.ds(own, NR), :].astype(jnp.float32).reshape(groups)
        acc_e = jnp.where(lanes == m - 1, turn(last, m), acc_e)
        acc_w = jnp.where(lanes == m, turn(first, m), acc_w)
    pk[0] = acc_e.reshape(NR, LN)
    pk[1] = acc_w.reshape(NR, LN)

    def side_by_side(dst, refs):
        for r in range(NR // SL):
            rows_e = pl.ds(pl.multiple_of(own + SL * r, SL), SL)
            acc_e = turn(refs[0][NC - 1, rows_e, :], HX)
            acc_w = refs[0][0, rows_e, :]
            for p, ref in enumerate(refs[1:], 1):
                here = lane >= p * HX
                acc_e = jnp.where(here, turn(ref[NC - 1, rows_e, :], HX * (p + 1)), acc_e)
                acc_w = jnp.where(here, turn(ref[0, rows_e, :], HX * p), acc_w)
            dst[0, pl.ds(SL * r, SL), :] = acc_e
            dst[1, pl.ds(SL * r, SL), :] = acc_w

    def sideways(src, dst, sends, recvs, from_row, to_row, rows):
        copies = []
        for d, side in enumerate((east, west)):
            copies.append(pltpu.make_async_remote_copy(
                src_ref=src.at[d], dst_ref=dst.at[d, pl.ds(own, NR), :],
                send_sem=sends.at[d, 0], recv_sem=recvs.at[d, 0],
                device_id={'col': side, 'row': row}, device_id_type=MESH))
            copies.append(pltpu.make_async_remote_copy(
                src_ref=src.at[d, pl.ds(from_row, rows), :], dst_ref=dst.at[d, pl.ds(to_row, rows), :],
                send_sem=sends.at[d, 1], recv_sem=recvs.at[d, 1],
                device_id={'col': side, 'row': other}, device_id_type=MESH))
        return copies

    corner = pl.multiple_of(PAD + HY - SL + (NR - HY + SL) * row, SL)
    x_copies = sideways(pk, rx, sem_xs, sem_xr, edge_src, corner, SL)
    for copy in x_copies:
        copy.start()
    side_by_side(pkw, (eta, ua, va, dep))

    for copy in flat_copies:
        copy.wait_recv()
    for r in range(STRIPS):
        cnt[0:NC, pl.ds(PAD + SL * r, SL), :] = cnt_i[:, pl.ds(PAD + SL * r, SL), :].astype(jnp.float32)


    def inner_half(h):
        for c in range(1, NC - 1):
            for f in range(len(cubes)):
                loads[f, c, h].wait()

    inner_half(0)
    w_copies = sideways(pkw, rxw, sem_ws, sem_wr, near, far, HY)
    for copy in w_copies:
        copy.start()
    for copy in row_copies:
        copy.wait_recv()

    half = 0.5 * BC_GRAVITY / LEVELS
    first0 = lax.broadcasted_iota(jnp.int32, (1, SL, LN), 2) == 0
    last127 = lax.broadcasted_iota(jnp.int32, (1, SL, LN), 2) == 127

    def shift_e(mine, following_tile):
        return roll_e(jnp.where(first0, following_tile, mine))

    def shift_w(mine, preceding_tile):
        return roll_w(jnp.where(last127, preceding_tile, mine))

    def ring_e(x):
        return shift_e(x, following(x))

    def ring_w(x):
        return shift_w(x, preceding(x))

    def inner(x):
        return x[1:3], x[2:4], x[0:2]

    def outer(x):
        return (jnp.concatenate([x[0:1], x[3:4]], axis=0), jnp.concatenate([x[1:2], x[4:5]], axis=0),
                jnp.concatenate([x[4:5], x[2:3]], axis=0))

    def every(x):
        return x[0:4], x[1:5], jnp.concatenate([x[4:5], x[0:3]], axis=0)

    def momentum(r, tiles, places):
        rb = pl.multiple_of(SL + SL * r, SL)
        eb = pl.multiple_of(own + SL * r, SL)
        out = pl.ds(pl.multiple_of(SL * r, SL), SL)
        y = (NR * row + SL * r + sub).astype(jnp.float32)
        fu4 = 0.25 * (CORIO_F0 + CORIO_BETA * ((y + 0.5) / (2 * NR) - 0.5))
        fv4 = 0.25 * (CORIO_F0 + CORIO_BETA * ((y + 1.0) / (2 * NR) - 0.5))

        def load(ref, k, dr=0):
            return ref[k, :, pl.ds(rb + dr, SL), :]

        def put(ref, rows, value):
            for i, c in enumerate(places):
                ref[c, rows, :] = value[i]

        count, count_e, _ = tiles(cnt[:, pl.ds(eb, SL), :])
        lu = jnp.minimum(count, shift_e(count, count_e))
        lv = jnp.minimum(count, tiles(cnt[:, pl.ds(eb + 1, SL), :])[0])
        qx = qy = su = sv = sdu = sdv = jnp.zeros((len(places), SL, LN), jnp.float32)
        wu = wv = None
        for k in range(LEVELS):
            u_all, un_all, v_all, vso_all = load(ub, k), load(ub, k, 1), load(vb, k), load(vb, k, -1)
            u, ue, uw = tiles(u_all)
            un, us = tiles(un_all)[0], tiles(load(ub, k, -1))[0]
            v, ve, vw = tiles(v_all)
            vn, vso = tiles(load(vb, k, 1))[0], tiles(vso_all)[0]
            rho, rho_e, _ = tiles((CONTRACT_S * half) * load(sb, k) - (EXPAND_T * half) * load(tb, k))
            rho_n = (CONTRACT_S * half) * tiles(load(sb, k, 1))[0] - (EXPAND_T * half) * tiles(load(tb, k, 1))[0]
            w2, w2_e, _ = tiles(v_all + vso_all)
            w4 = w2 + shift_e(w2, w2_e)
            y2, _, y2_w = tiles(u_all + un_all)
            y4 = y2 + shift_w(y2, y2_w)
            dx = shift_e(rho, rho_e) - rho
            dy = rho_n - rho
            px = qx + dx
            qx = px + dx
            py = qy + dy
            qy = py + dy
            du = w4 * (fu4 - 0.125 * (un - us)) - (0.5 * u) * (shift_e(u, ue) - shift_w(u, uw)) - px
            dv = -(y4 * (fv4 + 0.125 * (shift_e(v, ve) - shift_w(v, vw))) + (0.5 * v) * (vn - vso) + py)
            on_u = lu > float(k)
            on_v = lv > float(k)
            su = su + jnp.where(on_u, u, 0.0)
            sv = sv + jnp.where(on_v, v, 0.0)
            sdu = sdu + jnp.where(on_u, du, 0.0)
            sdv = sdv + jnp.where(on_v, dv, 0.0)
            tu, tv = u + du, v + dv
            wu = INV_V[k] * (tu if k == 0 else tu + VISC_R * wu)
            wv = INV_V[k] * (tv if k == 0 else tv + VISC_R * wv)
            put(vu.at[k], out, wu)
            put(vv.at[k], out, wv)
        inv_u = 1.0 / jnp.maximum(lu, 1.0)
        inv_v = 1.0 / jnp.maximum(lv, 1.0)
        depth, depth_e, _ = tiles(dep[:, pl.ds(eb, SL), :])
        hu = 0.5 * (depth + shift_e(depth, depth_e))
        hv = 0.5 * (depth + tiles(dep[:, pl.ds(eb + 1, SL), :])[0])
        put(fx, pl.ds(eb, SL), hu * (sdu * inv_u) / TIME_STEP)
        put(fy, pl.ds(eb, SL), hv * (sdv * inv_v) / TIME_STEP)
        put(meanu, out, (su + sdu) * inv_u)
        put(meanv, out, (sv + sdv) * inv_v)
        put(aux.at[0], out, count)
        put(aux.at[1], out, lu)
        put(aux.at[2], out, lv)

    def tracers(r):
        rb = pl.multiple_of(SL + SL * r, SL)
        eb = pl.multiple_of(own + SL * r, SL)
        out = pl.ds(pl.multiple_of(SL * r, SL), SL)

        def load(ref, k, dr=0):
            return ref[k, :, pl.ds(rb + dr, SL), :]

        count = cnt[:, pl.ds(eb, SL), :]
        lu = jnp.minimum(count, ring_e(count))
        count = count[:NC]
        lv = jnp.minimum(count, cnt[0:NC, pl.ds(eb + 1, SL), :])
        lvs = jnp.minimum(count, cnt[0:NC, pl.ds(eb - 1, SL), :])
        carried = [None, None]
        inside = count > 0.0
        for k in range(LEVELS):
            level = float(k)
            ge = TIME_STEP * jnp.where(lu > level, load(ub, k), 0.0)
            ge, _, gw = every(ge)
            gw = shift_w(ge, gw)
            gn = TIME_STEP * jnp.where(lv > level, load(vb, k)[:NC], 0.0)
            gs = TIME_STEP * jnp.where(lvs > level, load(vb, k, -1)[:NC], 0.0)
            keep = 2.0 - (ge - gw + gn - gs)
            inside_next = count > level + 1.0
            ending = 0.5 * INV_D[k] * END_D[k]
            pivot = ending if k == LEVELS - 1 else jnp.where(inside_next, 0.5 * INV_D[k], ending)
            for i, (buf, dst) in enumerate(((tb, vt), (sb, vs))):
                q, qe, qw = every(load(buf, k))
                twice = keep * q - (ge * shift_e(q, qe) - gw * shift_w(q, qw)
                                    + gn * load(buf, k, 1)[:NC] - gs * load(buf, k, -1)[:NC])
                w = pivot * (twice if k == 0 else twice + 2.0 * DIFF_R * carried[i])
                carried[i] = w
                dst[k, :, out, :] = jnp.where(inside, w, q)
            inside = inside_next

    @pl.loop(0, NR // SL)
    def _(r):
        @pl.when(r == part // SL - 1)
        def _():
            inner_half(1)

        momentum(r, inner, (1, 2))

    for copy in x_copies:
        copy.wait_recv()

    def unpack(rows, shape):
        even = lax.rem(lanes if len(shape) == 3 else lane, 2) == 0
        from_west, from_east = rx[0, rows, :].reshape(shape), rx[1, rows, :].reshape(shape)
        return jnp.where(even, from_east, from_west), jnp.where(even, from_west, from_east)

    def unpack_cube(f, rows, merged):
        for k in range(LEVELS):
            m = f * LEVELS + k
            cubes[f][1][k, NC, rows, :] = turn(merged[m % 2], -m).reshape(rows.size, LN)

    merged = unpack(pl.ds(own, NR), groups)
    for f in range(len(cubes)):
        unpack_cube(f, pl.ds(SL, NR), merged)
    cnt[NC, pl.ds(own, NR), :] = turn(merged[LANE_COUNT % 2], -LANE_COUNT).reshape(NR, LN)
    dep[NC, pl.ds(own, NR), :] = turn(merged[LANE_DEPTH % 2], -LANE_DEPTH).reshape(NR, LN)
    unpack_cube(1, pl.ds(0, SL), unpack(pl.ds(pl.multiple_of(own - SL, SL), SL), (SL, LN)))
    unpack_cube(0, pl.ds(SL + NR, SL), unpack(pl.ds(pl.multiple_of(own + NR, SL), SL), (SL, LN)))

    @pl.loop(0, NR // SL)
    def _(r):
        momentum(r, outer, (0, 3))

    side_by_side(pkl, (fx, fy, cnt))

    late = []
    for f, ref in enumerate((fx, fy)):
        late.append(pltpu.make_async_remote_copy(
            src_ref=ref.at[pl.ds(0, NC), pl.ds(mid, HY), :], dst_ref=ref.at[pl.ds(0, NC), pl.ds(far, HY), :],
            send_sem=sem_gs.at[f], recv_sem=sem_gr.at[f],
            device_id={'col': col, 'row': other}, device_id_type=MESH))
    late += sideways(pkl, rxl, sem_ls, sem_lr, near, far, HY)
    for copy in late:
        copy.start()

    @pl.loop(0, NR // SL)
    def _(r):
        tracers(r)

    for copy in w_copies + late:
        copy.wait_recv()
    weight_load.wait()

    def strip(r, dr=0):
        return pl.ds(PAD + SL * r + dr, SL)

    for r in range(STRIPS):
        for p, ref, src in ((0, eta, 1), (1, ua, 1), (2, va, 1), (3, dep, 1), (0, fx, 2), (1, fy, 2), (2, cnt, 2)):
            from_east = rxw[1, strip(r), :] if src == 1 else rxl[1, strip(r), :]
            from_west = rxw[0, strip(r), :] if src == 1 else rxl[0, strip(r), :]
            ref[NC, strip(r), :] = jnp.where(
                lane < HX, turn(from_east, -HX * p),
                jnp.where(lane >= LN - HX, turn(from_west, LN - HX - HX * p), 0.0))

    dt_fast = TIME_STEP / LEVELS
    for r in range(STRIPS):
        y = (HY * row + SL * r + sub).astype(jnp.float32)
        f_u = CORIO_F0 + CORIO_BETA * ((y + 0.5) / (2 * NR) - 0.5)
        f_v = CORIO_F0 + CORIO_BETA * ((y + 1.0) / (2 * NR) - 0.5)
        rows = strip(r)
        count, depth = cnt[:, rows, :], dep[:, rows, :]
        wet_u = (jnp.minimum(count, ring_e(count)) > 0.0).astype(jnp.float32)
        wet_v = (jnp.minimum(count, cnt[:, strip(r, 1), :]) > 0.0).astype(jnp.float32)
        mu[:, rows, :] = wet_u
        mv[:, rows, :] = wet_v
        au[:, rows, :] = wet_u * (0.25 * dt_fast * f_u)
        av[:, rows, :] = wet_v * (0.25 * dt_fast * f_v)
        bu[:, rows, :] = wet_u * (dt_fast * dt_fast) * fx[:, rows, :]
        bv[:, rows, :] = wet_v * (dt_fast * dt_fast) * fy[:, rows, :]
        scale = 0.5 * GRAVITY * dt_fast * dt_fast
        cu[:, rows, :] = wet_u * (scale * (depth + ring_e(depth)))
        cv[:, rows, :] = wet_v * (scale * (depth + dep[:, strip(r, 1), :]))
        ua[:, rows, :] = dt_fast * ua[:, rows, :]
        va[:, rows, :] = dt_fast * va[:, rows, :]
        accu[:, pl.ds(SL * r, SL), :] = jnp.zeros((NC, SL, LN), jnp.float32)
        accv[:, pl.ds(SL * r, SL), :] = jnp.zeros((NC, SL, LN), jnp.float32)

    def subcycle(n, u_old, v_old, u_new, v_new, span, first):
        weight = wts[n]
        weight_old = wts[jnp.maximum(n - 1, 0)]
        for r in span:
            rows = strip(r)
            u = u_old[:, rows, :]
            eta[:, rows, :] = eta[:, rows, :] - (u - ring_w(u) + v_old[:, rows, :] - v_old[:, strip(r, -1), :])
        for r in span:
            rows, rows_a = strip(r), pl.ds(SL * r, SL)
            u, v, e = u_old[:, rows, :], v_old[:, rows, :], eta[:, rows, :]
            w2 = v + v_old[:, strip(r, -1), :]
            y2 = u + u_old[:, strip(r, 1), :]
            ug, vg = (mu[:, rows, :] * u, mv[:, rows, :] * v) if first else (u, v)
            un = ug + (au[:, rows, :] * (w2 + ring_e(w2)) + bu[:, rows, :] - cu[:, rows, :] * (ring_e(e) - e))
            vn = vg + (bv[:, rows, :] - av[:, rows, :] * (y2 + ring_w(y2))
                       - cv[:, rows, :] * (eta[:, strip(r, 1), :] - e))
            u_new[:, rows, :] = un
            v_new[:, rows, :] = vn
            if u_new is ua:
                accu[:, rows_a, :] = accu[:, rows_a, :] + (weight_old * u[:NC] + weight * un[:NC])
                accv[:, rows_a, :] = accv[:, rows_a, :] + (weight_old * v[:NC] + weight * vn[:NC])

    def pair_of(pair, span, first):
        subcycle(2 * pair, ua, va, ubt, vbt, span, first)
        subcycle(2 * pair + 1, ubt, vbt, ua, va, span, False)

    pair_of(0, range(STRIPS), True)

    narrow = STRIPS - 2
    turning = (SL * (STRIPS - narrow) - 2) // 2

    def two_pairs(start, stop, span):
        @pl.loop(0, (stop - start) // 2)
        def _(q):
            for i in range(2):
                pair_of(start + 2 * q + i, span, False)

    two_pairs(1, turning, range(STRIPS))

    @pl.when(row == 0)
    def _():
        @pl.loop(turning, LEVELS // 2)
        def _(pair):
            pair_of(pair, range(narrow), False)

    @pl.when(row == 1)
    def _():
        @pl.loop(turning, LEVELS // 2)
        def _(pair):
            pair_of(pair, range(STRIPS - narrow, STRIPS), False)

    @pl.loop(0, NR // SL)
    def _(r):
        eb = pl.multiple_of(own + SL * r, SL)
        rows = pl.ds(eb, SL)
        rows_a = pl.ds(pl.multiple_of(eb - PAD, SL), SL)
        out = pl.ds(pl.multiple_of(SL * r, SL), SL)
        depth = dep[:, rows, :]
        hu = 0.5 * (depth + ring_e(depth))[:NC]
        hv = 0.5 * (depth + dep[:, pl.ds(eb + 1, SL), :])[:NC]
        aux[3, :, out, :] = LEVELS / TIME_STEP * accu[:, rows_a, :] / hu - meanu[:, out, :]
        aux[4, :, out, :] = LEVELS / TIME_STEP * accv[:, rows_a, :] / hv - meanv[:, out, :]
        aux[5, :, out, :] = eta[0:NC, rows, :]
        aux[6, :, out, :] = (LEVELS / TIME_STEP) * ua[0:NC, rows, :]
        aux[7, :, out, :] = (LEVELS / TIME_STEP) * va[0:NC, rows, :]

    for copy in row_copies + flat_copies + x_copies + w_copies + late:
        copy.wait_send()


def finish_kernel(vu, vv, vt, vs, aux, o_eta, o_tu, o_tv, o_u, o_v, o_t, o_s, *scratch):
    flat_bufs, cube_bufs, sem_f, sem_c = scratch[:3], scratch[3:7], scratch[7], scratch[8]
    flat_copies = []
    for i, (buf, ref) in enumerate(zip(flat_bufs, (o_eta, o_tu, o_tv))):
        for c in range(NC):
            buf[:, pl.ds(c * LN, LN)] = aux[5 + i, c]
        flat_copies.append(pltpu.make_async_copy(buf, ref, sem_f.at[i]))

    def copies(r):
        rows = pl.ds(SL * r if isinstance(r, int) else pl.multiple_of(SL * r, SL), SL)
        return [pltpu.make_async_copy(buf.at[:, rows, :], ref.at[:, rows, :], sem_c.at[i, r])
                for i, (buf, ref) in enumerate(zip(cube_bufs, (o_u, o_v, o_t, o_s)))]

    @pl.loop(0, NR // SL)
    def _(r):
        finish_rows(pl.ds(pl.multiple_of(SL * r, SL), SL), vu, vv, vt, vs, aux, *cube_bufs)
        for copy in copies(r):
            copy.start()

    for copy in flat_copies:
        copy.start()
    for r in range(NR // SL):
        for copy in copies(r):
            copy.wait()
    for copy in flat_copies:
        copy.wait()


def finish_rows(rows, vu, vv, vt, vs, aux, o_u, o_v, o_t, o_s):
    def put(ref, value):
        for c in range(NC):
            ref[rows, pl.ds(c * LN, LN)] = value[c]

    count, lu, lv, gu, gv = (aux[i, :, rows, :] for i in range(5))
    xu = xv = xt = xs = on_u = on_v = inside = None
    for k in reversed(range(LEVELS)):
        level = float(k)
        wu, wv, xt_new, xs_new = (ref[k, :, rows, :] for ref in (vu, vv, vt, vs))
        if k == LEVELS - 1:
            xu, xv = END_V[k] * wu, END_V[k] * wv
        else:
            xu = jnp.where(on_u, wu + CARRY_V[k] * xu, END_V[k] * wu)
            xv = jnp.where(on_v, wv + CARRY_V[k] * xv, END_V[k] * wv)
            xt_new = xt_new + CARRY_D[k] * jnp.where(inside, xt, 0.0)
            xs_new = xs_new + CARRY_D[k] * jnp.where(inside, xs, 0.0)
        xt, xs = xt_new, xs_new
        on_u, on_v, inside = lu > level, lv > level, count > level
        put(o_u.at[k], jnp.where(on_u, xu + gu, 0.0))
        put(o_v.at[k], jnp.where(on_v, xv + gv, 0.0))
        put(o_t.at[k], xt)
        put(o_s.at[k], xs)


def solution(mesh):
    n_col = mesh.shape['col']

    def step(vel_u, vel_v, temperature, salinity, surf_eta, trans_u, trans_v, bottom_depth, level_count, avg_weights):
        f32 = jnp.float32
        swept = jax.ShapeDtypeStruct((LEVELS, NC, NR, LN), f32)
        vmem = pl.BlockSpec(memory_space=pltpu.VMEM)
        anywhere = pl.BlockSpec(memory_space=pl.ANY)
        wide = pltpu.VMEM((NC + 1, EROWS, LN), f32)
        cube = pltpu.VMEM((LEVELS, NC + 1, NR + 16, LN), f32)
        acc = pltpu.VMEM((NC, EXT, LN), f32)
        mean = pltpu.VMEM((NC, NR, LN), f32)
        dma = pltpu.SemaphoreType.DMA
        swept_all = pl.pallas_call(
            functools.partial(step_kernel, n_col),
            out_shape=(swept,) * 4 + (jax.ShapeDtypeStruct((SL, NC, NR, LN), f32),),
            in_specs=[anywhere] * 10,
            out_specs=(vmem,) * 5,
            scratch_shapes=[cube] * 4 + [wide] * 7 + [pltpu.VMEM((NC, EROWS, LN), jnp.int32)] + [wide] * 10
            + [acc, acc, mean, mean,
               *[pltpu.VMEM((2, rows, LN), f32) for rows in (NR, NR, EROWS, EROWS, NR, EROWS)],
               pltpu.SMEM((LEVELS,), f32), dma(()), dma((4, NC - 2, 2))]
            + [dma((4, NC)), dma((5, NC)), dma((4, NC)), dma((4, NC)), dma((5, NC)), dma((5, NC)),
               *[dma((2, 2))] * 6, dma((2,)), dma((2,))],
            compiler_params=pltpu.CompilerParams(
                collective_id=0, has_side_effects=True, vmem_limit_bytes=33 * 1024 * 1024),
            name='step_kernel',
        )(*[pltpu.with_memory_space_constraint(x, pltpu.HBM) for x in (avg_weights, vel_u, vel_v, temperature, salinity, surf_eta, trans_u, trans_v, bottom_depth, level_count)])
        flat_out = jax.ShapeDtypeStruct(surf_eta.shape, f32)
        cube_out = jax.ShapeDtypeStruct(vel_u.shape, f32)
        return pl.pallas_call(
            finish_kernel,
            out_shape=(flat_out,) * 3 + (cube_out,) * 4,
            in_specs=[vmem] * 5,
            out_specs=(anywhere,) * 7,
            scratch_shapes=[pltpu.VMEM(surf_eta.shape, f32)] * 3 + [pltpu.VMEM(vel_u.shape, f32)] * 4
            + [dma((3,)), dma((4, NR // SL))],
            compiler_params=pltpu.CompilerParams(vmem_limit_bytes=20 * 1024 * 1024),
            name='finish_kernel',
        )(*swept_all)

    cube = P(None, 'row', 'col')
    flat = P('row', 'col')
    return jax.shard_map(step, mesh=mesh, in_specs=(cube, cube, cube, cube, flat, flat, flat, flat, flat, P()), out_specs=(flat, flat, flat, cube, cube, cube, cube), check_vma=False)
```
